8 devices in a mesh: f: 4 (over z, y, x), h: 2 (over core).
Axes of the slice: x: 2, y: 2, z: 1, core: 2. Of those that a mesh axis runs over, the one named last changes fastest.
Arguments:
- x: bfloat16 [64, 5120], P(None, 'h')
- g1: float32 [5120], P('h')
- g2: float32 [5120], P('h')
- w_gate: bfloat16 [5120, 13824], P('h', 'f')
- w_up: bfloat16 [5120, 13824], P('h', 'f')
- w_down: bfloat16 [13824, 5120], P('f', 'h')
- o: bfloat16 [64, 5120], P(None, 'f')
- w_o: bfloat16 [5120, 5120], P('f', 'h')
- w_qkv: bfloat16 [5120, 15360], P('h', 'f')
Outputs:
- output 1: bfloat16 [64, 5120], P(None, 'h')
- output 2: bfloat16 [64, 15360], P(None, 'f')
All inputs are finite; a program needn't handle non-finite values.
Results may differ from the reference program's by a relative error of at most 0.00390993.
Values are sent between devices in bfloat16 or wider.
A program may use at most 1 GiB of HBM per device.

```python
import jax
import jax.numpy as jnp
from jax import lax

T = 64
D = 5120
FF = 13824
HEADS = 40
KV_HEADS = 40
HEAD = 128
HD = HEADS * HEAD
Q = (HEADS + 2 * KV_HEADS) * HEAD
EPS = 1e-6


def _w(key, shape):
    return (jax.random.normal(key, shape, jnp.float32) * shape[0] ** -0.5).astype(jnp.bfloat16)


def setup_inputs(seed: int = 0) -> dict:
    ks = jax.random.split(jax.random.PRNGKey(seed), 11)
    z = jax.random.normal(ks[0], (T, D), jnp.float32)
    row = jnp.exp(jax.random.uniform(ks[1], (T, 1), jnp.float32, -1.0, 1.0))
    tilt = jax.random.uniform(ks[2], (T, 1), jnp.float32, -1.0, 1.0)
    pos = jnp.arange(D, dtype=jnp.float32)[None, :] * (2.0 / D) - 1.0
    x = (z * row * jnp.exp(tilt * pos)).astype(jnp.bfloat16)
    o = (0.7 * jax.random.normal(ks[8], (T, HD), jnp.float32)).astype(jnp.bfloat16)
    return {
        'x': x,
        'g1': jax.random.uniform(ks[3], (D,), jnp.float32, 0.5, 1.5),
        'g2': jax.random.uniform(ks[4], (D,), jnp.float32, 0.5, 1.5),
        'w_gate': _w(ks[5], (D, FF)),
        'w_up': _w(ks[6], (D, FF)),
        'w_down': _w(ks[7], (FF, D)),
        'o': o,
        'w_o': _w(ks[9], (HD, D)),
        'w_qkv': _w(ks[10], (D, Q)),
    }


def _norm(x, g):
    xf = x.astype(jnp.float32)
    r = lax.rsqrt(jnp.mean(xf * xf, axis=-1, keepdims=True) + EPS)
    return (xf * r * g).astype(jnp.bfloat16)


def reference(x, g1, g2, w_gate, w_up, w_down, o, w_o, w_qkv):
    n = _norm(x, g1)
    gt = jnp.dot(n, w_gate, preferred_element_type=jnp.float32)
    up = jnp.dot(n, w_up, preferred_element_type=jnp.float32)
    a = (jax.nn.silu(gt) * up).astype(jnp.bfloat16)
    y = jnp.dot(a, w_down, preferred_element_type=jnp.float32) + jnp.dot(o, w_o, preferred_element_type=jnp.float32)
    x_next = (x.astype(jnp.float32) + y).astype(jnp.bfloat16)
    n1 = _norm(x_next, g2)
    qkv = jnp.dot(n1, w_qkv, preferred_element_type=jnp.float32).astype(jnp.bfloat16)
    return (x_next, qkv)
```

```python
import functools

import jax
import jax.numpy as jnp
from jax import lax
from jax.experimental import pallas as pl
from jax.experimental.pallas import tpu as pltpu
from jax.sharding import PartitionSpec as P

EPS = 1e-6
MESH = pl.DeviceIdType.MESH
F32, BF16 = jnp.float32, jnp.bfloat16


def _dot(a, b):
    return jnp.dot(a, b, preferred_element_type=F32)


def _kernel(cfg, x_hbm, g1_hbm, g2_hbm, wg_hbm, wu_hbm, wd_hbm, o_hbm, wo_hbm, wq_hbm,
            xo_hbm, qo_hbm,
            ring, wdv, xv, gv, oa, nv, xnv, ss1, ss2, pown, prec, ysend, yrec, qown, qrec, qout,
            s_in, s_wg, s_wu, s_wd, s_wo, s_wq, s_out,
            c_ss, c_p, c_y_s, c_y_r, c_x_s, c_x_r, c_s2_s, c_s2_r, c_q):
    d, kd, ko, slots, half, ng, cw, ny, qw, nq, rows = cfg
    f, h = lax.axis_index('f'), lax.axis_index('h')
    partner = (f, 1 - h)
    fx = [f, f + 1 - 2 * lax.rem(f, 2), lax.rem(f + 2, 4), 3 - f]

    def small():
        return [pltpu.make_async_copy(x_hbm, xv, s_in.at[0]),
                pltpu.make_async_copy(g1_hbm, gv.at[pl.ds(0, 1)], s_in.at[1]),
                pltpu.make_async_copy(g2_hbm, gv.at[pl.ds(1, 1)], s_in.at[2]),
                pltpu.make_async_copy(o_hbm, oa.at[:, pl.ds(0, ko)], s_in.at[3])]

    def gu(j):
        slot, cols = lax.rem(j, slots), pl.ds(pl.multiple_of(j * half, 128), half)
        return [pltpu.make_async_copy(wg_hbm.at[:, cols], ring.at[slot, :, pl.ds(0, half)], s_wg.at[j]),
                pltpu.make_async_copy(wu_hbm.at[:, cols], ring.at[slot, :, pl.ds(half, half)], s_wu.at[j])]

    def dn(c):
        cols = pl.ds(pl.multiple_of(c * cw, 128), cw)
        return [pltpu.make_async_copy(wo_hbm.at[:, cols], wdv.at[c, pl.ds(0, ko)], s_wo.at[c]),
                pltpu.make_async_copy(wd_hbm.at[:, cols], wdv.at[c, pl.ds(ko, kd)], s_wd.at[c])]

    def qk(j):
        slot, cols = lax.rem(j + ng, slots), pl.ds(pl.multiple_of(j * qw, 128), qw)
        return [pltpu.make_async_copy(wq_hbm.at[:, cols], ring.at[slot], s_wq.at[j])]

    def start(copies):
        for c in copies:
            c.start()

    def wait(copies):
        for c in copies:
            c.wait()

    ins = small()
    start(ins)
    for j in range(slots):
        start(gu(j))

    barrier = pltpu.get_barrier_semaphore()
    for k in range(4):
        for t in range(2):
            if k or t:
                pl.semaphore_signal(barrier, inc=1, device_id=(fx[k], h if t == 0 else 1 - h), device_id_type=MESH)

    wait(ins)
    xf = xv[...].astype(F32)
    s = jnp.sum(xf * xf, axis=-1, keepdims=True)
    ss1[h] = jnp.broadcast_to(s, ss1.shape[1:])
    pl.semaphore_wait(barrier, 7)
    ex = pltpu.make_async_remote_copy(ss1.at[h], ss1.at[h], c_ss.at[0], c_ss.at[1], partner, MESH)
    ex.start()
    ex.wait()
    r = lax.rsqrt((ss1[0] + ss1[1])[:, :1] / (2 * d) + EPS)
    nv[...] = (xv[...].astype(F32) * r * gv[0:1, :]).astype(BF16)

    def pcopy(j):
        return pltpu.make_async_remote_copy(pown.at[j], prec.at[j], c_p.at[0, j], c_p.at[1, j], partner, MESH)

    def act(j):
        pcopy(j).wait_recv()
        g = pown[j, :, :half] + prec[j, :, :half]
        u = pown[j, :, half:] + prec[j, :, half:]
        oa[:, pl.ds(pl.multiple_of(ko + j * half, 128), half)] = (g / (1.0 + jnp.exp(-g)) * u).astype(BF16)

    def gu_step(j, _):
        wait(gu(j))
        pown[j] = _dot(nv[...], ring[lax.rem(j, slots)])
        pcopy(j).start()

        @pl.when(j + slots < ng)
        def _():
            start(gu(j + slots))

        @pl.when(j + slots == ng - 1)
        def _():
            for c in range(ny):
                start(dn(c))

        @pl.when((j + slots >= ng) & (j + slots < ng + nq))
        def _():
            start(qk(j + slots - ng))

        @pl.when(j > 0)
        def _():
            act(j - 1)
        return 0

    lax.fori_loop(0, ng, gu_step, 0)
    act(ng - 1)

    def ycopy(c, k):
        blk = pl.ds(pl.multiple_of(fx[k] * rows, rows), rows)
        return pltpu.make_async_remote_copy(ysend.at[c, blk], yrec.at[k - 1, c], c_y_s.at[k - 1, c], c_y_r.at[k - 1, c],
                                            (fx[k], h), MESH)

    def dn_step(c, _):
        wait(dn(c))
        ysend[c] = _dot(oa[...], wdv[c])
        for k in (3, 1, 2):
            ycopy(c, k).start()
        return 0

    lax.fori_loop(0, ny, dn_step, 0)

    mine = pl.ds(pl.multiple_of(f * rows, rows), rows)

    def xcopy(c, k):
        cols = pl.ds(c * cw, cw)
        return pltpu.make_async_remote_copy(xnv.at[mine, cols], xnv.at[mine, cols], c_x_s.at[k - 1, c], c_x_r.at[k - 1, c],
                                            (fx[k], h), MESH)

    s = jnp.zeros((rows, 1), F32)
    for c in range(ny):
        for k in (1, 2, 3):
            ycopy(c, k).wait_recv()
        y = (ysend[c, mine] + yrec[0, c]) + (yrec[1, c] + yrec[2, c])
        xn = (xv[mine, c * cw:(c + 1) * cw].astype(F32) + y).astype(BF16)
        xnv[mine, c * cw:(c + 1) * cw] = xn
        xf = xn.astype(F32)
        s = s + jnp.sum(xf * xf, axis=-1, keepdims=True)
        if c < ny - 1:
            for k in (3, 1, 2):
                xcopy(c, k).start()
    ss2[h, mine] = jnp.broadcast_to(s, (rows, 128))

    def scopy(k, t):
        i = k * 2 + t - 1
        return pltpu.make_async_remote_copy(ss2.at[h, mine], ss2.at[h, mine], c_s2_s.at[i], c_s2_r.at[i],
                                            (fx[k], h if t == 0 else 1 - h), MESH)

    peers = [(k, t) for k in (3, 1, 2, 0) for t in (0, 1) if k or t]
    for k, t in peers:
        scopy(k, t).start()
    for k in (3, 1, 2):
        xcopy(ny - 1, k).start()
    for k, t in peers:
        scopy(k, t).wait_recv()
    r = lax.rsqrt((ss2[0] + ss2[1])[:, :1] / (2 * d) + EPS)
    for c in range(ny):
        for k in (1, 2, 3):
            xcopy(c, k).wait_recv()
        cols = slice(c * cw, (c + 1) * cw)
        nv[:, cols] = (xnv[:, cols].astype(F32) * r * gv[1:2, cols]).astype(BF16)
    xout = pltpu.make_async_copy(xnv, xo_hbm, s_out.at[nq])
    xout.start()

    def qcopy(j):
        return pltpu.make_async_remote_copy(qown.at[j], qrec.at[j], c_q.at[0, j], c_q.at[1, j], partner, MESH)

    def oput(j):
        cols = pl.ds(pl.multiple_of(j * qw, 128), qw)
        return pltpu.make_async_copy(qout.at[:, cols], qo_hbm.at[:, cols], s_out.at[j])

    def fin(j):
        qcopy(j).wait_recv()
        qout[:, pl.ds(pl.multiple_of(j * qw, 128), qw)] = (qown[j] + qrec[j]).astype(BF16)
        oput(j).start()

    def q_step(j, _):
        wait(qk(j))
        qown[j] = _dot(nv[...], ring[lax.rem(j + ng, slots)])
        qcopy(j).start()

        @pl.when(j > 0)
        def _():
            fin(j - 1)
        return 0

    lax.fori_loop(0, nq, q_step, 0)
    fin(nq - 1)

    for j in range(ng):
        pcopy(j).wait_send()
    for c in range(ny):
        for k in (1, 2, 3):
            ycopy(c, k).wait_send()
            xcopy(c, k).wait_send()
    for k, t in peers:
        scopy(k, t).wait_send()
    for j in range(nq):
        qcopy(j).wait_send()
        oput(j).wait()
    xout.wait()


def solution(mesh):
    def body(x, g1, g2, w_gate, w_up, w_down, o, w_o, w_qkv):
        t, d = x.shape
        kd, ko, q = w_down.shape[0], w_o.shape[0], w_qkv.shape[1]
        slots, half, cw, qw = 6, 384, 512, 768
        ng, ny, nq, rows = kd // half, d // cw, q // qw, t // 4
        cfg = (d, kd, ko, slots, half, ng, cw, ny, qw, nq, rows)
        dma = pltpu.SemaphoreType.DMA
        any_ = pl.BlockSpec(memory_space=pl.ANY)
        return pl.pallas_call(
            functools.partial(_kernel, cfg),
            out_shape=(jax.ShapeDtypeStruct((t, d), BF16), jax.ShapeDtypeStruct((t, q), BF16)),
            in_specs=[any_] * 9,
            out_specs=(any_, any_),
            scratch_shapes=[
                pltpu.VMEM((slots, d, 2 * half), BF16),
                pltpu.VMEM((ny, ko + kd, cw), BF16),
                pltpu.VMEM((t, d), BF16),
                pltpu.VMEM((2, d), F32),
                pltpu.VMEM((t, ko + kd), BF16),
                pltpu.VMEM((t, d), BF16),
                pltpu.VMEM((t, d), BF16),
                pltpu.VMEM((2, t, 128), F32),
                pltpu.VMEM((2, t, 128), F32),
                pltpu.VMEM((ng, t, 2 * half), F32),
                pltpu.VMEM((ng, t, 2 * half), F32),
                pltpu.VMEM((ny, t, cw), F32),
                pltpu.VMEM((3, ny, rows, cw), F32),
                pltpu.VMEM((nq, t, qw), F32),
                pltpu.VMEM((nq, t, qw), F32),
                pltpu.VMEM((t, q), BF16),
                dma((4,)), dma((ng,)), dma((ng,)), dma((ny,)), dma((ny,)), dma((nq,)), dma((nq + 1,)),
                dma((2,)), dma((2, ng)), dma((3, ny)), dma((3, ny)), dma((3, ny)), dma((3, ny)),
                dma((7,)), dma((7,)), dma((2, nq)),
            ],
            compiler_params=pltpu.CompilerParams(collective_id=0, has_side_effects=True,
                                                 vmem_limit_bytes=66_000_000),
            name='block',
        )(x, g1.reshape(1, -1), g2.reshape(1, -1), w_gate, w_up, w_down, o, w_o, w_qkv)

    in_specs = (P(None, 'h'), P('h'), P('h'), P('h', 'f'), P('h', 'f'), P('f', 'h'),
                P(None, 'f'), P('f', 'h'), P('h', 'f'))
    return jax.shard_map(body, mesh=mesh, in_specs=in_specs,
                         out_specs=(P(None, 'h'), P(None, 'f')), check_vma=False)
```

```python
import functools

import jax
import jax.numpy as jnp
from jax import lax
from jax.experimental import pallas as pl
from jax.experimental.pallas import tpu as pltpu
from jax.sharding import PartitionSpec as P

EPS = 1e-6
MESH = pl.DeviceIdType.MESH
F32, BF16 = jnp.float32, jnp.bfloat16


def _dot(a, b):
    return jnp.dot(a, b, preferred_element_type=F32)


def _kernel(cfg, x_hbm, g1_hbm, g2_hbm, wg_hbm, wu_hbm, wd_hbm, o_hbm, wo_hbm, wq_hbm,
            xnv, qout,
            ring, wdv, xv, gv, oa, nv, ss1, ss2, pown, prec, ysend, yrec, qown, qrec,
            s_in, s_wg, s_wu, s_wd, s_wo, s_wq,
            c_ss, c_p, c_y_s, c_y_r, c_x_s, c_x_r, c_s2_s, c_s2_r, c_q):
    d, kd, ko, slots, half, ng, cw, ny, qw, nq, rows = cfg
    f, h = lax.axis_index('f'), lax.axis_index('h')
    partner = (f, 1 - h)
    fx = [f, f + 1 - 2 * lax.rem(f, 2), lax.rem(f + 2, 4), 3 - f]

    def small():
        return [pltpu.make_async_copy(x_hbm, xv, s_in.at[0]),
                pltpu.make_async_copy(g1_hbm, gv.at[0], s_in.at[1]),
                pltpu.make_async_copy(g2_hbm, gv.at[1], s_in.at[2]),
                pltpu.make_async_copy(o_hbm, oa.at[:, pl.ds(0, ko)], s_in.at[3])]

    def gu(j):
        slot, cols = lax.rem(j, slots), pl.ds(pl.multiple_of(j * half, 128), half)
        return [pltpu.make_async_copy(wg_hbm.at[:, cols], ring.at[slot, :, pl.ds(0, half)], s_wg.at[j]),
                pltpu.make_async_copy(wu_hbm.at[:, cols], ring.at[slot, :, pl.ds(half, half)], s_wu.at[j])]

    def dn(c):
        cols = pl.ds(pl.multiple_of(c * cw, 128), cw)
        return [pltpu.make_async_copy(wo_hbm.at[:, cols], wdv.at[c, pl.ds(0, ko)], s_wo.at[c]),
                pltpu.make_async_copy(wd_hbm.at[:, cols], wdv.at[c, pl.ds(ko, kd)], s_wd.at[c])]

    def qk(j):
        slot, cols = lax.rem(j + ng, slots), pl.ds(pl.multiple_of(j * qw, 128), qw)
        return [pltpu.make_async_copy(wq_hbm.at[:, cols], ring.at[slot], s_wq.at[j])]

    def start(copies, priority):
        for c in copies:
            c.start(priority=priority)

    def wait(copies):
        for c in copies:
            c.wait()

    def loop(lo, hi, fn):
        lax.fori_loop(lo, hi, lambda i, _: (fn(i), 0)[1], 0)

    ins = small()
    start(ins, 0)
    loop(0, slots, lambda j: start(gu(j), 0))
    loop(0, ny, lambda c: start(dn(c), 1))

    barrier = pltpu.get_barrier_semaphore()
    for k in range(4):
        for t in range(2):
            if k or t:
                pl.semaphore_signal(barrier, inc=1, device_id=(fx[k], h if t == 0 else 1 - h), device_id_type=MESH)

    wait(ins)
    xf = xv[...].astype(F32)
    s = jnp.sum(xf * xf, axis=-1, keepdims=True)
    ss1[h] = jnp.broadcast_to(s, ss1.shape[1:])
    pl.semaphore_wait(barrier, 7)
    ex = pltpu.make_async_remote_copy(ss1.at[h], ss1.at[h], c_ss.at[0], c_ss.at[1], partner, MESH)
    ex.start()
    ex.wait()
    r = lax.rsqrt((ss1[0] + ss1[1])[:, :1] / (2 * d) + EPS)
    for i in range(d // 128):
        cols = slice(i * 128, (i + 1) * 128)
        nv[:, cols] = (xv[:, cols].astype(F32) * r * gv[0, i:i + 1, :]).astype(BF16)

    def pcopy(j):
        return pltpu.make_async_remote_copy(pown.at[j], prec.at[j], c_p.at[0, j], c_p.at[1, j], partner, MESH)

    def act(j):
        pcopy(j).wait_recv()
        g = pown[j, :, :half] + prec[j, :, :half]
        u = pown[j, :, half:] + prec[j, :, half:]
        oa[:, pl.ds(pl.multiple_of(ko + j * half, 128), half)] = (g / (1.0 + jnp.exp(-g)) * u).astype(BF16)

    def gu_step(j, _):
        wait(gu(j))
        pown[j] = _dot(nv[...], ring[lax.rem(j, slots)])
        pcopy(j).start()

        @pl.when(j + slots < ng)
        def _():
            start(gu(j + slots), 0)

        @pl.when(j > 1)
        def _():
            act(j - 2)
        return 0

    lax.fori_loop(0, ng, gu_step, 0)
    loop(0, nq, lambda j: start(qk(j), 1))
    act(ng - 2)
    act(ng - 1)

    def ycopy(c, k):
        blk = pl.ds(pl.multiple_of(fx[k] * rows, rows), rows)
        return pltpu.make_async_remote_copy(ysend.at[c, blk], yrec.at[k - 1, c], c_y_s.at[k - 1, c], c_y_r.at[k - 1, c],
                                            (fx[k], h), MESH)

    def dn_step(c, _):
        wait(dn(c))

        ysend[c] = _dot(oa[...], wdv[c])
        for k in (3, 1, 2):
            ycopy(c, k).start()
        return 0

    lax.fori_loop(0, ny, dn_step, 0)

    mine = pl.ds(pl.multiple_of(f * rows, rows), rows)

    def xcopy(c, k):
        cols = pl.ds(c * cw, cw)
        return pltpu.make_async_remote_copy(xnv.at[mine, cols], xnv.at[mine, cols], c_x_s.at[k - 1, c], c_x_r.at[k - 1, c],
                                            (fx[k], h), MESH)

    s = jnp.zeros((rows, 1), F32)
    for c in range(ny):
        for k in (1, 2, 3):
            ycopy(c, k).wait_recv()
        y = (ysend[c, mine] + yrec[0, c]) + (yrec[1, c] + yrec[2, c])
        xn = (xv[mine, c * cw:(c + 1) * cw].astype(F32) + y).astype(BF16)
        xnv[mine, c * cw:(c + 1) * cw] = xn
        xf = xn.astype(F32)
        s = s + jnp.sum(xf * xf, axis=-1, keepdims=True)
        if c < ny - 1:
            for k in (3, 1, 2):
                xcopy(c, k).start()
    ss2[h, mine] = jnp.broadcast_to(s, (rows, 128))

    def scopy(k, t):
        i = k * 2 + t - 1
        return pltpu.make_async_remote_copy(ss2.at[h, mine], ss2.at[h, mine], c_s2_s.at[i], c_s2_r.at[i],
                                            (fx[k], h if t == 0 else 1 - h), MESH)

    peers = [(k, t) for k in (3, 1, 2, 0) for t in (0, 1) if k or t]
    for k, t in peers:
        scopy(k, t).start()
    for k in (3, 1, 2):
        xcopy(ny - 1, k).start()
    for k, t in peers:
        scopy(k, t).wait_recv()
    r = lax.rsqrt((ss2[0] + ss2[1])[:, :1] / (2 * d) + EPS)
    for c in range(ny):
        for k in (1, 2, 3):
            xcopy(c, k).wait_recv()
        for i in range(c * cw // 128, (c + 1) * cw // 128):
            cols = slice(i * 128, (i + 1) * 128)
            nv[:, cols] = (xnv[:, cols].astype(F32) * r * gv[1, i:i + 1, :]).astype(BF16)

    def qcopy(j):
        return pltpu.make_async_remote_copy(qown.at[j], qrec.at[j], c_q.at[0, j], c_q.at[1, j], partner, MESH)

    def fin(j):
        qcopy(j).wait_recv()
        qout[:, pl.ds(pl.multiple_of(j * qw, 128), qw)] = (qown[j] + qrec[j]).astype(BF16)

    def q_step(j, _):
        wait(qk(j))
        qown[j] = _dot(nv[...], ring[lax.rem(j + ng, slots)])
        qcopy(j).start()

        @pl.when(j > 1)
        def _():
            fin(j - 2)
        return 0

    lax.fori_loop(0, nq, q_step, 0)
    fin(nq - 2)
    fin(nq - 1)

    for j in range(ng):
        pcopy(j).wait_send()
    for c in range(ny):
        for k in (1, 2, 3):
            ycopy(c, k).wait_send()
            xcopy(c, k).wait_send()
    for k, t in peers:
        scopy(k, t).wait_send()
    for j in range(nq):
        qcopy(j).wait_send()


def _store(x_ref, q_ref, xo_hbm, qo_hbm, sem):
    cx = pltpu.make_async_copy(x_ref, xo_hbm, sem.at[0])
    cq = pltpu.make_async_copy(q_ref, qo_hbm, sem.at[1])
    cx.start()
    cq.start()
    cx.wait()
    cq.wait()


def solution(mesh):
    def body(x, g1, g2, w_gate, w_up, w_down, o, w_o, w_qkv):
        t, d = x.shape
        kd, ko, q = w_down.shape[0], w_o.shape[0], w_qkv.shape[1]
        slots, half, cw, qw = 6, 384, 512, 768
        ng, ny, nq, rows = kd // half, d // cw, q // qw, t // 4
        cfg = (d, kd, ko, slots, half, ng, cw, ny, qw, nq, rows)
        dma = pltpu.SemaphoreType.DMA
        any_ = pl.BlockSpec(memory_space=pl.ANY)
        vmem = pl.BlockSpec(memory_space=pltpu.VMEM)
        outs = (jax.ShapeDtypeStruct((t, d), BF16), jax.ShapeDtypeStruct((t, q), BF16))
        mids = (pltpu.VMEM((t, d), BF16), pltpu.VMEM((t, q), BF16))
        res = pl.pallas_call(
            functools.partial(_kernel, cfg),
            out_shape=mids,
            in_specs=[any_] * 9,
            out_specs=(vmem, vmem),
            scratch_shapes=[
                pltpu.VMEM((slots, d, 2 * half), BF16),
                pltpu.VMEM((ny, ko + kd, cw), BF16),
                pltpu.VMEM((t, d), BF16),
                pltpu.VMEM((2, d // 128, 128), F32),
                pltpu.VMEM((t, ko + kd), BF16),
                pltpu.VMEM((t, d), BF16),
                pltpu.VMEM((2, t, 128), F32),
                pltpu.VMEM((2, t, 128), F32),
                pltpu.VMEM((ng, t, 2 * half), F32),
                pltpu.VMEM((ng, t, 2 * half), F32),
                pltpu.VMEM((ny, t, cw), F32),
                pltpu.VMEM((3, ny, rows, cw), F32),
                pltpu.VMEM((nq, t, qw), F32),
                pltpu.VMEM((nq, t, qw), F32),
                dma((4,)), dma((ng,)), dma((ng,)), dma((ny,)), dma((ny,)), dma((nq,)),
                dma((2,)), dma((2, ng)), dma((3, ny)), dma((3, ny)), dma((3, ny)), dma((3, ny)),
                dma((7,)), dma((7,)), dma((2, nq)),
            ],
            compiler_params=pltpu.CompilerParams(collective_id=0, has_side_effects=True,
                                                 vmem_limit_bytes=60_000_000),
            name='block',
        )(x, g1.reshape(-1, 128), g2.reshape(-1, 128), w_gate, w_up, w_down, o, w_o, w_qkv)
        return pl.pallas_call(_store, out_shape=outs, in_specs=[vmem, vmem], out_specs=(any_, any_),
                              scratch_shapes=[dma((2,))], name='store')(*[pltpu.with_memory_space_constraint(r, pltpu.VMEM) for r in res])

    in_specs = (P(None, 'h'), P('h'), P('h'), P('h', 'f'), P('h', 'f'), P('f', 'h'),
                P(None, 'f'), P('f', 'h'), P('h', 'f'))
    return jax.shard_map(body, mesh=mesh, in_specs=in_specs,
                         out_specs=(P(None, 'h'), P(None, 'f')), check_vma=False)
```

```python
import functools

import jax
import jax.numpy as jnp
from jax import lax
from jax.experimental import pallas as pl
from jax.experimental.pallas import tpu as pltpu
from jax.sharding import PartitionSpec as P

EPS = 1e-6
MESH = pl.DeviceIdType.MESH
F32, BF16 = jnp.float32, jnp.bfloat16


def _dot(a, b):
    return jnp.dot(a, b, preferred_element_type=F32)


def _kernel(cfg, x_hbm, g1_hbm, g2_hbm, wg_hbm, wu_hbm, wd_hbm, o_hbm, wo_hbm, wq_hbm,
            xnv, qout,
            ring, wdv, xv, gv, oa, nv, ss1, ss2, pown, prec, ysend, yrec, qown, qrec,
            s_in, s_wg, s_wu, s_wd, s_wo, s_wq,
            c_ss, c_p, c_y, c_x, c_s2, c_q, c_sent):
    d, kd, ko, slots, half, ng, nl, cw, ny, qw, nq, rows = cfg
    f, h = lax.axis_index('f'), lax.axis_index('h')
    partner = (f, 1 - h)
    fx = [f, f + 1 - 2 * lax.rem(f, 2), lax.rem(f + 2, 4), 3 - f]

    def small():
        return [pltpu.make_async_copy(x_hbm, xv, s_in.at[0]),
                pltpu.make_async_copy(g1_hbm, gv.at[0], s_in.at[1]),
                pltpu.make_async_copy(g2_hbm, gv.at[1], s_in.at[2]),
                pltpu.make_async_copy(o_hbm, oa.at[:, pl.ds(0, ko)], s_in.at[3])]

    def gu(j):
        slot, cols = lax.rem(j, slots), pl.ds(pl.multiple_of(j * half, 128), half)
        return [pltpu.make_async_copy(wg_hbm.at[:, cols], ring.at[slot, :, pl.ds(0, half)], s_wg.at[j]),
                pltpu.make_async_copy(wu_hbm.at[:, cols], ring.at[slot, :, pl.ds(half, half)], s_wu.at[j])]

    def gl(e):
        cols = pl.ds(pl.multiple_of(ng * half + e * 128, 128), 128)
        lo, hi = pl.multiple_of(e * 256, 128), pl.multiple_of(e * 256 + 128, 128)
        return [pltpu.make_async_copy(wg_hbm.at[:, cols], ring.at[ng % slots, :, pl.ds(lo, 128)], s_wg.at[ng + e]),
                pltpu.make_async_copy(wu_hbm.at[:, cols], ring.at[ng % slots, :, pl.ds(hi, 128)], s_wu.at[ng + e])]

    def dn(c):
        cols = pl.ds(pl.multiple_of(c * cw, 128), cw)
        return [pltpu.make_async_copy(wo_hbm.at[:, cols], wdv.at[c, pl.ds(0, ko)], s_wo.at[c]),
                pltpu.make_async_copy(wd_hbm.at[:, cols], wdv.at[c, pl.ds(ko, kd)], s_wd.at[c])]

    def qk(j):
        slot, cols = lax.rem(j + ng + 1, slots), pl.ds(pl.multiple_of(j * qw, 128), qw)
        return [pltpu.make_async_copy(wq_hbm.at[:, cols], ring.at[slot], s_wq.at[j])]

    def took(ref, sem):
        pltpu.make_async_copy(ref, ref, sem).wait()

    def start(copies, priority):
        for c in copies:
            c.start(priority=priority)

    def wait(copies):
        for c in copies:
            c.wait()

    def loop(lo, hi, fn):
        lax.fori_loop(lo, hi, lambda i, _: (fn(i), 0)[1], 0)

    ins = small()
    start(ins, 0)
    loop(0, slots, lambda j: start(gu(j), 0))
    loop(0, ny, lambda c: start(dn(c), 1))

    barrier = pltpu.get_barrier_semaphore()
    for k in range(4):
        for t in range(2):
            if k or t:
                pl.semaphore_signal(barrier, inc=1, device_id=(fx[k], h if t == 0 else 1 - h), device_id_type=MESH)

    wait(ins)
    xf = xv[...].astype(F32)
    s = jnp.sum(xf * xf, axis=-1, keepdims=True)
    ss1[h] = jnp.broadcast_to(s, ss1.shape[1:])
    pl.semaphore_wait(barrier, 7)
    ex = pltpu.make_async_remote_copy(ss1.at[h], ss1.at[h], c_ss.at[0], c_ss.at[1], partner, MESH)
    ex.start()
    ex.wait()
    r = lax.rsqrt((ss1[0] + ss1[1])[:, :1] / (2 * d) + EPS)
    for i in range(d // 128):
        cols = slice(i * 128, (i + 1) * 128)
        nv[:, cols] = (xv[:, cols].astype(F32) * r * gv[0, i:i + 1, :]).astype(BF16)

    def pcopy(j):
        return pltpu.make_async_remote_copy(pown.at[j], prec.at[j], c_sent.at[0], c_p.at[j], partner, MESH)

    def lcopy(e):
        part = pl.ds(pl.multiple_of(e * 256, 128), 256)
        return pltpu.make_async_remote_copy(pown.at[ng, :, part], prec.at[ng, :, part], c_sent.at[1], c_p.at[ng + e],
                                            partner, MESH)

    def silu_mul(g, u):
        return (g / (1.0 + jnp.exp(-g)) * u).astype(BF16)

    def act(j):
        pcopy(j).wait_recv()
        oa[:, pl.ds(pl.multiple_of(ko + j * half, 128), half)] = silu_mul(pown[j, :, :half] + prec[j, :, :half],
                                                                          pown[j, :, half:] + prec[j, :, half:])

    def last_act(e):
        lcopy(e).wait_recv()
        lo, hi = (pl.ds(pl.multiple_of(e * 256 + i, 128), 128) for i in (0, 128))
        oa[:, pl.ds(pl.multiple_of(ko + ng * half + e * 128, 128), 128)] = silu_mul(
            pown[ng, :, lo] + prec[ng, :, lo], pown[ng, :, hi] + prec[ng, :, hi])

    def gu_step(j, _):
        wait(gu(j))
        pown[j] = _dot(nv[...], ring[lax.rem(j, slots)])
        pcopy(j).start()

        @pl.when(j + slots < ng)
        def _():
            start(gu(j + slots), 0)

        @pl.when(j + slots == ng)
        def _():
            loop(0, nl, lambda e: start(gl(e), 0))

        @pl.when(j > 1)
        def _():
            act(j - 2)
        return 0

    def gl_step(e, _):
        wait(gl(e))
        part = pl.ds(pl.multiple_of(e * 256, 128), 256)
        pown[ng, :, part] = _dot(nv[...], ring[ng % slots, :, part])
        lcopy(e).start()
        return 0

    lax.fori_loop(0, ng, gu_step, 0)
    lax.fori_loop(0, nl, gl_step, 0)
    loop(0, nq, lambda j: start(qk(j), 1))

    blk = [pl.ds(pl.multiple_of(fx[k] * rows, rows), rows) for k in range(4)]
    mine = blk[0]

    def chunk(c):
        return pl.ds(pl.multiple_of(c * cw, 128), cw)

    def ycopy(c, k):
        return pltpu.make_async_remote_copy(ysend.at[c, blk[k]], yrec.at[k - 1, c], c_sent.at[2], c_y.at[c],
                                            (fx[k], h), MESH)

    def xcopy(c, k):
        return pltpu.make_async_remote_copy(xnv.at[mine, chunk(c)], xnv.at[mine, chunk(c)], c_sent.at[3],
                                            c_x.at[0], (fx[k], h), MESH)

    def scatter(c):
        for k in (3, 1, 2):
            ycopy(c, k).start()

    act(ng - 2)
    wait(dn(0))
    kk = ko + (ng - 1) * half
    ysend[0] = _dot(oa[:, :kk], wdv[0, :kk])
    act(ng - 1)
    loop(0, nl, last_act)
    ysend[0] = ysend[0] + _dot(oa[:, kk:], wdv[0, kk:])
    scatter(0)

    def dn_step(c, _):
        wait(dn(c))
        ysend[c] = _dot(oa[...], wdv[c])
        scatter(c)
        return 0

    lax.fori_loop(1, ny, dn_step, 0)

    def block(c, s):
        took(yrec.at[:, c], c_y.at[c])
        y = (ysend[c, mine] + yrec[0, c]) + (yrec[1, c] + yrec[2, c])
        xn = (xv[mine, chunk(c)].astype(F32) + y).astype(BF16)
        xnv[mine, chunk(c)] = xn

        @pl.when(c < ny - 2)
        def _():
            for k in (3, 1, 2):
                xcopy(c, k).start()

        xf = xn.astype(F32)
        return s + jnp.sum(xf * xf, axis=-1, keepdims=True)

    s = lax.fori_loop(0, ny, block, jnp.zeros((rows, 1), F32))

    def diag(n, first):
        i = lax.broadcasted_iota(jnp.int32, (n, 128), 0) + first
        return i == lax.broadcasted_iota(jnp.int32, (n, 128), 1)

    ss2[h * 4 + f] = jnp.sum(jnp.where(diag(rows, f * rows), s, 0.0), axis=0, keepdims=True)

    def scopy(k, t):
        return pltpu.make_async_remote_copy(ss2.at[h * 4 + f], ss2.at[h * 4 + f], c_sent.at[5], c_s2.at[0],
                                            (fx[k], h if t == 0 else 1 - h), MESH)

    peers = [(k, t) for k in (3, 1, 2, 0) for t in (0, 1) if k or t]
    for k, t in peers:
        scopy(k, t).start()
    for c in (ny - 2, ny - 1):
        for k in (3, 1, 2):
            xcopy(c, k).start()
    took(pown.at[pl.ds(0, ng)], c_sent.at[0])
    took(pown.at[ng], c_sent.at[1])
    took(ysend.at[:, pl.ds(0, 3 * rows)], c_sent.at[2])
    took(ss2.at[pl.ds(0, 7)], c_sent.at[5])
    took(ss2.at[pl.ds(0, 7)], c_s2.at[0])
    tot = sum(ss2[i] + ss2[4 + i] for i in range(4))
    tot = jnp.sum(jnp.where(diag(4 * rows, 0), tot, 0.0), axis=1, keepdims=True)
    r = lax.rsqrt(tot / (2 * d) + EPS)

    took(xnv.at[pl.ds(0, 3 * rows)], c_x.at[0])

    def renorm(c):
        for i in range(cw // 128):
            cols = pl.ds(pl.multiple_of(c * cw + i * 128, 128), 128)
            nv[:, cols] = (xnv[:, cols].astype(F32) * r * gv[1, pl.ds(c * (cw // 128) + i, 1), :]).astype(BF16)

    loop(0, ny, renorm)

    def qcopy(j):
        return pltpu.make_async_remote_copy(qown.at[j], qrec.at[j], c_sent.at[4], c_q.at[j], partner, MESH)

    def fin(j):
        qcopy(j).wait_recv()
        qout[:, pl.ds(pl.multiple_of(j * qw, 128), qw)] = (qown[j] + qrec[j]).astype(BF16)

    def q_pair(i, _):
        wait(qk(2 * i) + qk(2 * i + 1))
        for j in (2 * i, 2 * i + 1):
            qown[j] = _dot(nv[...], ring[lax.rem(j + ng + 1, slots)])
        for j in (2 * i, 2 * i + 1):
            qcopy(j).start()

        @pl.when(i > 0)
        def _():
            fin(2 * i - 2)
            fin(2 * i - 1)
        return 0

    lax.fori_loop(0, nq // 2, q_pair, 0)
    wait(qk(nq - 1))
    qown[nq - 1] = _dot(nv[...], ring[(nq + ng) % slots])
    qcopy(nq - 1).start()
    for j in range(nq - 3, nq):
        fin(j)

    took(xnv.at[pl.ds(0, 3 * rows)], c_sent.at[3])
    took(qown, c_sent.at[4])


def _store(x_ref, q_ref, xo_hbm, qo_hbm, sem):
    cx = pltpu.make_async_copy(x_ref, xo_hbm, sem.at[0])
    cq = pltpu.make_async_copy(q_ref, qo_hbm, sem.at[1])
    cx.start()
    cq.start()
    cx.wait()
    cq.wait()


def solution(mesh):
    def body(x, g1, g2, w_gate, w_up, w_down, o, w_o, w_qkv):
        t, d = x.shape
        kd, ko, q = w_down.shape[0], w_o.shape[0], w_qkv.shape[1]
        slots, half, nl, cw, qw = 6, 384, 3, 256, 768
        ng, ny, nq, rows = kd // half - 1, d // cw, q // qw, t // 4
        cfg = (d, kd, ko, slots, half, ng, nl, cw, ny, qw, nq, rows)
        dma = pltpu.SemaphoreType.DMA
        any_ = pl.BlockSpec(memory_space=pl.ANY)
        vmem = pl.BlockSpec(memory_space=pltpu.VMEM)
        outs = (jax.ShapeDtypeStruct((t, d), BF16), jax.ShapeDtypeStruct((t, q), BF16))
        mids = (pltpu.VMEM((t, d), BF16), pltpu.VMEM((t, q), BF16))
        res = pl.pallas_call(
            functools.partial(_kernel, cfg),
            out_shape=mids,
            in_specs=[any_] * 9,
            out_specs=(vmem, vmem),
            scratch_shapes=[
                pltpu.VMEM((slots, d, 2 * half), BF16),
                pltpu.VMEM((ny, ko + kd, cw), BF16),
                pltpu.VMEM((t, d), BF16),
                pltpu.VMEM((2, d // 128, 128), F32),
                pltpu.VMEM((t, ko + kd), BF16),
                pltpu.VMEM((t, d), BF16),
                pltpu.VMEM((2, t, 128), F32),
                pltpu.VMEM((8, 1, 128), F32),
                pltpu.VMEM((ng + 1, t, 2 * half), F32),
                pltpu.VMEM((ng + 1, t, 2 * half), F32),
                pltpu.VMEM((ny, t, cw), F32),
                pltpu.VMEM((3, ny, rows, cw), F32),
                pltpu.VMEM((nq, t, qw), F32),
                pltpu.VMEM((nq, t, qw), F32),
                dma((4,)), dma((ng + nl,)), dma((ng + nl,)), dma((ny,)), dma((ny,)), dma((nq,)),
                dma((2,)), dma((ng + nl,)), dma((ny,)), dma((1,)), dma((1,)), dma((nq,)), dma((6,)),
            ],
            compiler_params=pltpu.CompilerParams(collective_id=0, has_side_effects=True,
                                                 vmem_limit_bytes=60_000_000),
            name='block',
        )(x, g1.reshape(-1, 128), g2.reshape(-1, 128), w_gate, w_up, w_down, o, w_o, w_qkv)
        return pl.pallas_call(_store, out_shape=outs, in_specs=[vmem, vmem], out_specs=(any_, any_),
                              scratch_shapes=[dma((2,))], name='store')(*[pltpu.with_memory_space_constraint(r, pltpu.VMEM) for r in res])

    in_specs = (P(None, 'h'), P('h'), P('h'), P('h', 'f'), P('h', 'f'), P('f', 'h'),
                P(None, 'f'), P('f', 'h'), P('h', 'f'))
    return jax.shard_map(body, mesh=mesh, in_specs=in_specs,
                         out_specs=(P(None, 'h'), P(None, 'f')), check_vma=False)
```

```python
import functools

import jax
import jax.numpy as jnp
from jax import lax
from jax.experimental import pallas as pl
from jax.experimental.pallas import tpu as pltpu
from jax.sharding import PartitionSpec as P

EPS = 1e-6
MESH = pl.DeviceIdType.MESH
F32, BF16 = jnp.float32, jnp.bfloat16


def _dot(a, b):
    return jnp.dot(a, b, preferred_element_type=F32)


def _kernel(cfg, x_hbm, g1_hbm, g2_hbm, wg_hbm, wu_hbm, wd_hbm, o_hbm, wo_hbm, wq_hbm,
            xnv, qout,
            ring, wdv, xv, gv, oa, nv, ss1, ss2, pown, prec, ysend, yrec, qown, qrec,
            s_in, s_w, s_dn,
            c_ss, c_p, c_y, c_x, c_s2, c_q, c_sent):
    d, kd, ko, slots, half, ng, nl, cw, ny, qw, nq, rows = cfg
    f, h = lax.axis_index('f'), lax.axis_index('h')
    partner = (f, 1 - h)
    fx = [f, f + 1 - 2 * lax.rem(f, 2), lax.rem(f + 2, 4), 3 - f]

    def small():
        return [pltpu.make_async_copy(x_hbm, xv, s_in.at[0]),
                pltpu.make_async_copy(g1_hbm, gv.at[0], s_in.at[1]),
                pltpu.make_async_copy(g2_hbm, gv.at[1], s_in.at[1]),
                pltpu.make_async_copy(o_hbm, oa.at[:, pl.ds(0, ko)], s_in.at[2])]

    def gu(j):
        slot, cols = lax.rem(j, slots), pl.ds(pl.multiple_of(j * half, 128), half)
        return [pltpu.make_async_copy(wg_hbm.at[:, cols], ring.at[slot, :, pl.ds(0, half)], s_w.at[slot]),
                pltpu.make_async_copy(wu_hbm.at[:, cols], ring.at[slot, :, pl.ds(half, half)], s_w.at[slot])]

    def gl(e):
        cols = pl.ds(pl.multiple_of(ng * half + e * 128, 128), 128)
        lo, hi = pl.multiple_of(e * 256, 128), pl.multiple_of(e * 256 + 128, 128)
        return [pltpu.make_async_copy(wg_hbm.at[:, cols], ring.at[ng % slots, :, pl.ds(lo, 128)], s_w.at[slots + e]),
                pltpu.make_async_copy(wu_hbm.at[:, cols], ring.at[ng % slots, :, pl.ds(hi, 128)], s_w.at[slots + e])]

    def dn(c):
        cols = pl.ds(pl.multiple_of(c * cw, 128), cw)
        return [pltpu.make_async_copy(wo_hbm.at[:, cols], wdv.at[c, pl.ds(0, ko)], s_dn.at[c]),
                pltpu.make_async_copy(wd_hbm.at[:, cols], wdv.at[c, pl.ds(ko, kd)], s_dn.at[c])]

    def qk(j):
        slot, cols = lax.rem(j + ng + 1, slots), pl.ds(pl.multiple_of(j * qw, 128), qw)
        return [pltpu.make_async_copy(wq_hbm.at[:, cols], ring.at[slot], s_w.at[slot])]

    def took(ref, sem):
        pltpu.make_async_copy(ref, ref, sem).wait()

    def start(copies, priority):
        for c in copies:
            c.start(priority=priority)

    def wait(copies):
        for c in copies:
            c.wait()

    def loop(lo, hi, fn):
        lax.fori_loop(lo, hi, lambda i, _: (fn(i), 0)[1], 0)

    ins = small()
    start(ins, 0)
    loop(0, slots, lambda j: start(gu(j), 0))
    loop(0, ny, lambda c: start(dn(c), 1))

    barrier = pltpu.get_barrier_semaphore()
    for k in range(4):
        for t in range(2):
            if k or t:
                pl.semaphore_signal(barrier, inc=1, device_id=(fx[k], h if t == 0 else 1 - h), device_id_type=MESH)

    took(xv, s_in.at[0])
    xf = xv[...].astype(F32)
    s = jnp.sum(xf * xf, axis=-1, keepdims=True)
    ss1[h] = jnp.broadcast_to(s, ss1.shape[1:])
    pl.semaphore_wait(barrier, 7)
    ex = pltpu.make_async_remote_copy(ss1.at[h], ss1.at[h], c_ss.at[0], c_ss.at[1], partner, MESH)
    ex.start()
    ex.wait()
    r = lax.rsqrt((ss1[0] + ss1[1])[:, :1] / (2 * d) + EPS)
    took(gv, s_in.at[1])
    for i in range(d // 128):
        cols = slice(i * 128, (i + 1) * 128)
        nv[:, cols] = (xv[:, cols].astype(F32) * r * gv[0, i:i + 1, :]).astype(BF16)

    def pcopy(j):
        return pltpu.make_async_remote_copy(pown.at[j], prec.at[j], c_sent.at[0], c_p.at[j], partner, MESH)

    def lcopy(e):
        part = pl.ds(pl.multiple_of(e * 256, 128), 256)
        return pltpu.make_async_remote_copy(pown.at[ng, :, part], prec.at[ng, :, part], c_sent.at[0], c_p.at[ng],
                                            partner, MESH)

    def silu_mul(g, u):
        return (g / (1.0 + jnp.exp(-g)) * u).astype(BF16)

    def act(j):
        pcopy(j).wait_recv()
        oa[:, pl.ds(pl.multiple_of(ko + j * half, 128), half)] = silu_mul(pown[j, :, :half] + prec[j, :, :half],
                                                                          pown[j, :, half:] + prec[j, :, half:])

    def last_act(e):
        lo, hi = (pl.ds(pl.multiple_of(e * 256 + i, 128), 128) for i in (0, 128))
        oa[:, pl.ds(pl.multiple_of(ko + ng * half + e * 128, 128), 128)] = silu_mul(
            pown[ng, :, lo] + prec[ng, :, lo], pown[ng, :, hi] + prec[ng, :, hi])

    def gu_step(j, _):
        took(ring.at[lax.rem(j, slots)], s_w.at[lax.rem(j, slots)])
        pown[j] = _dot(nv[...], ring[lax.rem(j, slots)])
        pcopy(j).start()

        @pl.when(j + slots < ng)
        def _():
            start(gu(j + slots), 0)

        @pl.when(j + slots == ng)
        def _():
            loop(0, nl, lambda e: start(gl(e), 0))

        @pl.when(j > 1)
        def _():
            act(j - 2)
        return 0

    def gl_step(e, _):
        part = pl.ds(pl.multiple_of(e * 256, 128), 256)
        took(ring.at[ng % slots, :, part], s_w.at[slots + e])
        pown[ng, :, part] = _dot(nv[...], ring[ng % slots, :, part])
        lcopy(e).start()
        return 0

    lax.fori_loop(0, ng, gu_step, 0)
    lax.fori_loop(0, nl, gl_step, 0)
    loop(0, nq, lambda j: start(qk(j), 1))

    blk = [pl.ds(pl.multiple_of(fx[k] * rows, rows), rows) for k in range(4)]
    mine = blk[0]

    def chunk(c):
        return pl.ds(pl.multiple_of(c * cw, 128), cw)

    def ycopy(c, k):
        return pltpu.make_async_remote_copy(ysend.at[c, blk[k]], yrec.at[k - 1, c], c_sent.at[1], c_y.at[c],
                                            (fx[k], h), MESH)

    def xcopy(c, k):
        at = xnv.at[mine, chunk(c)]
        return pltpu.make_async_remote_copy(at, at, c_sent.at[2], c_x.at[lax.div(c, ny // 2)], (fx[k], h), MESH)

    def spread(c):
        for k in (3, 1, 2):
            xcopy(c, k).start()

    def scatter(c):
        for k in (3, 1, 2):
            ycopy(c, k).start()

    act(ng - 2)
    ins[3].wait()
    took(wdv.at[0], s_dn.at[0])
    kk = ko + (ng - 1) * half
    ysend[0] = _dot(oa[:, :kk], wdv[0, :kk])
    act(ng - 1)
    took(prec.at[ng], c_p.at[ng])
    loop(0, nl, last_act)
    ysend[0] = ysend[0] + _dot(oa[:, kk:], wdv[0, kk:])
    scatter(0)

    def dn_step(c, _):
        took(wdv.at[c], s_dn.at[c])
        ysend[c] = _dot(oa[...], wdv[c])
        scatter(c)
        return 0

    lax.fori_loop(1, ny, dn_step, 0)

    def block(c, s):
        took(yrec.at[:, c], c_y.at[c])
        y = (ysend[c, mine] + yrec[0, c]) + (yrec[1, c] + yrec[2, c])
        xn = (xv[mine, chunk(c)].astype(F32) + y).astype(BF16)
        xnv[mine, chunk(c)] = xn

        @pl.when(c < ny // 2)
        def _():
            spread(c)

        xf = xn.astype(F32)
        return s + jnp.sum(xf * xf, axis=-1, keepdims=True)

    s = lax.fori_loop(0, ny, block, jnp.zeros((rows, 1), F32))

    def diag(n, first):
        i = lax.broadcasted_iota(jnp.int32, (n, 128), 0) + first
        return i == lax.broadcasted_iota(jnp.int32, (n, 128), 1)

    ss2[h * 4 + f] = jnp.sum(jnp.where(diag(rows, f * rows), s, 0.0), axis=0, keepdims=True)

    def scopy(k, t):
        return pltpu.make_async_remote_copy(ss2.at[h * 4 + f], ss2.at[h * 4 + f], c_sent.at[4], c_s2.at[0],
                                            (fx[k], h if t == 0 else 1 - h), MESH)

    peers = [(k, t) for k in (3, 1, 2, 0) for t in (0, 1) if k or t]
    for k, t in peers:
        scopy(k, t).start()
    loop(ny // 2, ny, spread)
    qown[...] = jnp.zeros_like(qown)
    took(pown, c_sent.at[0])
    took(ysend.at[:, pl.ds(0, 3 * rows)], c_sent.at[1])
    took(ss2.at[pl.ds(0, 7)], c_sent.at[4])
    took(ss2.at[pl.ds(0, 7)], c_s2.at[0])
    tot = sum(ss2[i] + ss2[4 + i] for i in range(4))
    tot = jnp.sum(jnp.where(diag(4 * rows, 0), tot, 0.0), axis=1, keepdims=True)
    r = lax.rsqrt(tot / (2 * d) + EPS)


    def renorm(c):
        for i in range(cw // 128):
            cols = pl.ds(pl.multiple_of(c * cw + i * 128, 128), 128)
            nv[:, cols] = (xnv[:, cols].astype(F32) * r * gv[1, pl.ds(c * (cw // 128) + i, 1), :]).astype(BF16)

    def qcopy(j):
        return pltpu.make_async_remote_copy(qown.at[j], qrec.at[j], c_sent.at[3], c_q.at[lax.div(j, 2)], partner, MESH)

    def fin(j):
        qout[:, pl.ds(pl.multiple_of(j * qw, 128), qw)] = (qown[j] + qrec[j]).astype(BF16)

    def q_pass(p, _):
        took(xnv.at[pl.ds(0, 3 * rows), pl.ds(0, d // 2)], c_x.at[p])
        loop(p * (ny // 2), (p + 1) * (ny // 2), renorm)
        ks = pl.ds(pl.multiple_of(p * (d // 2), 128), d // 2)

        def add(*js):
            @pl.when(p == 0)
            def _():
                for j in js:
                    wait(qk(j))

            for j in js:
                qown[j] = qown[j] + _dot(nv[:, ks], ring[lax.rem(j + ng + 1, slots), ks])

            @pl.when(p == 1)
            def _():
                for j in js:
                    qcopy(j).start()

        def q_pair(i, _):
            add(2 * i, 2 * i + 1)
            return 0

        lax.fori_loop(0, nq // 2, q_pair, 0)
        add(nq - 1)
        return 0

    lax.fori_loop(0, 2, q_pass, 0)

    def fin_pair(i):
        took(qrec.at[pl.ds(0, 2)], c_q.at[i])
        fin(2 * i)
        fin(2 * i + 1)

    loop(0, nq // 2, fin_pair)
    took(qrec.at[0], c_q.at[nq // 2])
    fin(nq - 1)

    took(xnv.at[pl.ds(0, 3 * rows)], c_sent.at[2])
    took(qown, c_sent.at[3])


def _store(x_ref, q_ref, xo_hbm, qo_hbm, sem):
    cx = pltpu.make_async_copy(x_ref, xo_hbm, sem.at[0])
    cq = pltpu.make_async_copy(q_ref, qo_hbm, sem.at[1])
    cx.start()
    cq.start()
    cx.wait()
    cq.wait()


def solution(mesh):
    def body(x, g1, g2, w_gate, w_up, w_down, o, w_o, w_qkv):
        t, d = x.shape
        kd, ko, q = w_down.shape[0], w_o.shape[0], w_qkv.shape[1]
        slots, half, nl, cw, qw = 6, 384, 3, 256, 768
        ng, ny, nq, rows = kd // half - 1, d // cw, q // qw, t // 4
        cfg = (d, kd, ko, slots, half, ng, nl, cw, ny, qw, nq, rows)
        dma = pltpu.SemaphoreType.DMA
        any_ = pl.BlockSpec(memory_space=pl.ANY)
        vmem = pl.BlockSpec(memory_space=pltpu.VMEM)
        outs = (jax.ShapeDtypeStruct((t, d), BF16), jax.ShapeDtypeStruct((t, q), BF16))
        mids = (pltpu.VMEM((t, d), BF16), pltpu.VMEM((t, q), BF16))
        res = pl.pallas_call(
            functools.partial(_kernel, cfg),
            out_shape=mids,
            in_specs=[any_] * 9,
            out_specs=(vmem, vmem),
            scratch_shapes=[
                pltpu.VMEM((slots, d, 2 * half), BF16),
                pltpu.VMEM((ny, ko + kd, cw), BF16),
                pltpu.VMEM((t, d), BF16),
                pltpu.VMEM((2, d // 128, 128), F32),
                pltpu.VMEM((t, ko + kd), BF16),
                pltpu.VMEM((t, d), BF16),
                pltpu.VMEM((2, t, 128), F32),
                pltpu.VMEM((8, 1, 128), F32),
                pltpu.VMEM((ng + 1, t, 2 * half), F32),
                pltpu.VMEM((ng + 1, t, 2 * half), F32),
                pltpu.VMEM((ny, t, cw), F32),
                pltpu.VMEM((3, ny, rows, cw), F32),
                pltpu.VMEM((nq, t, qw), F32),
                pltpu.VMEM((nq, t, qw), F32),
                dma((3,)), dma((slots + nl,)), dma((ny,)),
                dma((2,)), dma((ng + 1,)), dma((ny,)), dma((2,)), dma((1,)), dma(((nq + 1) // 2,)), dma((5,)),
            ],
            compiler_params=pltpu.CompilerParams(collective_id=0, has_side_effects=True,
                                                 vmem_limit_bytes=60_000_000),
            name='block',
        )(x, g1.reshape(-1, 128), g2.reshape(-1, 128), w_gate, w_up, w_down, o, w_o, w_qkv)
        return pl.pallas_call(_store, out_shape=outs, in_specs=[vmem, vmem], out_specs=(any_, any_),
                              scratch_shapes=[dma((2,))], name='store')(*[pltpu.with_memory_space_constraint(r, pltpu.VMEM) for r in res])

    in_specs = (P(None, 'h'), P('h'), P('h'), P('h', 'f'), P('h', 'f'), P('f', 'h'),
                P(None, 'f'), P('f', 'h'), P('h', 'f'))
    return jax.shard_map(body, mesh=mesh, in_specs=in_specs,
                         out_specs=(P(None, 'h'), P(None, 'f')), check_vma=False)
```

```python
import functools

import jax
import jax.numpy as jnp
from jax import lax
from jax.experimental import pallas as pl
from jax.experimental.pallas import tpu as pltpu
from jax.sharding import PartitionSpec as P

EPS = 1e-6
MESH = pl.DeviceIdType.MESH
F32, BF16 = jnp.float32, jnp.bfloat16


def _dot(a, b):
    return jnp.dot(a, b, preferred_element_type=F32)


def _kernel(cfg, x_hbm, g1_hbm, g2_hbm, wg_hbm, wu_hbm, wd_hbm, o_hbm, wo_hbm, wq_hbm,
            xnv, qout,
            ring, wdv, xv, gv, oa, nv, ss1, ss2, pown, prec, ysend, yrec, qown, qrec,
            s_in, s_w, s_dn,
            c_ss, c_p, c_y, c_x, c_s2, c_q, c_sent):
    d, kd, ko, slots, half, ng, nm, cw, ny, qw, nq, rows = cfg
    f, h = lax.axis_index('f'), lax.axis_index('h')
    partner = (f, 1 - h)
    fx = [f, f + 1 - 2 * lax.rem(f, 2), lax.rem(f + 2, 4), 3 - f]

    def small():
        return [pltpu.make_async_copy(x_hbm, xv, s_in.at[0]),
                pltpu.make_async_copy(g1_hbm, gv.at[0], s_in.at[1]),
                pltpu.make_async_copy(g2_hbm, gv.at[1], s_in.at[1]),
                pltpu.make_async_copy(o_hbm, oa.at[:, pl.ds(0, ko)], s_in.at[2])]

    def wide(j):
        return j, pl.multiple_of(j * half, 128), half

    def mid(m):
        return ng + m, pl.multiple_of(ng * half + m * 256, 128), 256

    last = (ng + nm, ng * half + nm * 256, 128)

    def gu(i, at, w):
        slot, cols = lax.rem(i, slots), pl.ds(at, w)
        return [pltpu.make_async_copy(wg_hbm.at[:, cols], ring.at[slot, :, pl.ds(0, w)], s_w.at[slot]),
                pltpu.make_async_copy(wu_hbm.at[:, cols], ring.at[slot, :, pl.ds(w, w)], s_w.at[slot])]

    def dn(c):
        cols = pl.ds(pl.multiple_of(c * cw, 128), cw)
        return [pltpu.make_async_copy(wo_hbm.at[:, cols], wdv.at[c, pl.ds(0, ko)], s_dn.at[c]),
                pltpu.make_async_copy(wd_hbm.at[:, cols], wdv.at[c, pl.ds(ko, kd)], s_dn.at[c])]

    def qk(j):
        slot, cols = lax.rem(j + ng + nm + 1, slots), pl.ds(pl.multiple_of(j * qw, 128), qw)
        return [pltpu.make_async_copy(wq_hbm.at[:, cols], ring.at[slot], s_w.at[slot])]

    def took(ref, sem):
        pltpu.make_async_copy(ref, ref, sem).wait()

    def start(copies, priority):
        for c in copies:
            c.start(priority=priority)

    def wait(copies):
        for c in copies:
            c.wait()

    def loop(lo, hi, fn):
        lax.fori_loop(lo, hi, lambda i, _: (fn(i), 0)[1], 0)

    ins = small()
    start(ins, 0)
    loop(0, ng, lambda j: start(gu(*wide(j)), 0))
    loop(0, ny, lambda c: start(dn(c), 1))

    barrier = pltpu.get_barrier_semaphore()
    for k in range(4):
        for t in range(2):
            if k or t:
                pl.semaphore_signal(barrier, inc=1, device_id=(fx[k], h if t == 0 else 1 - h), device_id_type=MESH)

    took(xv, s_in.at[0])
    xf = xv[...].astype(F32)
    s = jnp.sum(xf * xf, axis=-1, keepdims=True)
    ss1[h] = jnp.broadcast_to(s, ss1.shape[1:])
    pl.semaphore_wait(barrier, 7)
    ex = pltpu.make_async_remote_copy(ss1.at[h], ss1.at[h], c_ss.at[0], c_ss.at[1], partner, MESH)
    ex.start()
    ex.wait()
    r = lax.rsqrt((ss1[0] + ss1[1])[:, :1] / (2 * d) + EPS)
    took(gv, s_in.at[1])
    for i in range(d // 128):
        cols = slice(i * 128, (i + 1) * 128)
        nv[:, cols] = (xv[:, cols].astype(F32) * r * gv[0, i:i + 1, :]).astype(BF16)

    def pcopy(i, w):
        part = pl.ds(0, 2 * w)
        return pltpu.make_async_remote_copy(pown.at[i, :, part], prec.at[i, :, part],
                                            c_sent.at[0 if w == half else (5 if w == 256 else 6)], c_p.at[i], partner, MESH)

    def act(i, at, w):
        took(prec.at[i, :, pl.ds(0, 2 * w)], c_p.at[i])
        g = pown[i, :, :w] + prec[i, :, :w]
        u = pown[i, :, w:2 * w] + prec[i, :, w:2 * w]
        oa[:, pl.ds(pl.multiple_of(ko + at, 128), w)] = (g / (1.0 + jnp.exp(-g)) * u).astype(BF16)

    def product(i, at, w):
        slot, part = lax.rem(i, slots), pl.ds(0, 2 * w)
        took(ring.at[slot, :, part], s_w.at[slot])
        pown[i, :, part] = _dot(nv[...], ring[slot, :, part])
        pcopy(i, w).start()

    def gu_step(j, _):
        product(*wide(j))

        @pl.when(j < nm)
        def _():
            start(gu(*mid(j)), 0)

        @pl.when(j == nm)
        def _():
            start(gu(*last), 0)

        @pl.when(j > 1)
        def _():
            act(*wide(j - 2))
        return 0

    def mid_step(m, _):
        product(*mid(m))

        @pl.when(m < 2)
        def _():
            act(*wide(ng - 2 + m))
        return 0

    lax.fori_loop(0, ng, gu_step, 0)
    lax.fori_loop(0, nm, mid_step, 0)
    product(*last)
    loop(0, nq, lambda j: start(qk(j), 1))

    blk = [pl.ds(pl.multiple_of(fx[k] * rows, rows), rows) for k in range(4)]
    mine = blk[0]

    def chunk(c):
        return pl.ds(pl.multiple_of(c * cw, 128), cw)

    def ycopy(c, k):
        return pltpu.make_async_remote_copy(ysend.at[c, blk[k]], yrec.at[k - 1, c], c_sent.at[1], c_y.at[c],
                                            (fx[k], h), MESH)

    def xcopy(c, k):
        at = xnv.at[mine, chunk(c)]
        return pltpu.make_async_remote_copy(at, at, c_sent.at[2], c_x.at[lax.div(c, ny // 2)], (fx[k], h), MESH)

    def spread(c):
        for k in (3, 1, 2):
            xcopy(c, k).start()

    def scatter(c):
        for k in (3, 1, 2):
            ycopy(c, k).start()

    loop(0, nm - 2, lambda m: act(*mid(m)))
    ins[3].wait()
    took(wdv.at[0], s_dn.at[0])
    kk = ko + ng * half + (nm - 2) * 256
    ysend[0] = _dot(oa[:, :kk], wdv[0, :kk])
    loop(nm - 2, nm, lambda m: act(*mid(m)))
    act(*last)
    ysend[0] = ysend[0] + _dot(oa[:, kk:], wdv[0, kk:])
    scatter(0)

    def dn_step(c, _):
        took(wdv.at[c], s_dn.at[c])
        ysend[c] = _dot(oa[...], wdv[c])
        scatter(c)
        return 0

    lax.fori_loop(1, ny, dn_step, 0)

    def block(c, s):
        took(yrec.at[:, c], c_y.at[c])
        y = (ysend[c, mine] + yrec[0, c]) + (yrec[1, c] + yrec[2, c])
        xn = (xv[mine, chunk(c)].astype(F32) + y).astype(BF16)
        xnv[mine, chunk(c)] = xn

        @pl.when(c < ny // 2)
        def _():
            spread(c)

        xf = xn.astype(F32)
        return s + jnp.sum(xf * xf, axis=-1, keepdims=True)

    s = lax.fori_loop(0, ny, block, jnp.zeros((rows, 1), F32))

    def diag(n, first):
        i = lax.broadcasted_iota(jnp.int32, (n, 128), 0) + first
        return i == lax.broadcasted_iota(jnp.int32, (n, 128), 1)

    ss2[h * 4 + f] = jnp.sum(jnp.where(diag(rows, f * rows), s, 0.0), axis=0, keepdims=True)

    def scopy(k, t):
        return pltpu.make_async_remote_copy(ss2.at[h * 4 + f], ss2.at[h * 4 + f], c_sent.at[4], c_s2.at[0],
                                            (fx[k], h if t == 0 else 1 - h), MESH)

    peers = [(k, t) for k in (3, 1, 2, 0) for t in (0, 1) if k or t]
    for k, t in peers:
        scopy(k, t).start()
    loop(ny // 2, ny, spread)
    qown[...] = jnp.zeros_like(qown)
    took(pown.at[pl.ds(0, ng)], c_sent.at[0])
    took(pown.at[pl.ds(0, nm), :, pl.ds(0, 512)], c_sent.at[5])
    took(pown.at[0, :, pl.ds(0, 256)], c_sent.at[6])
    took(ysend.at[:, pl.ds(0, 3 * rows)], c_sent.at[1])
    took(ss2.at[pl.ds(0, 7)], c_sent.at[4])
    took(ss2.at[pl.ds(0, 7)], c_s2.at[0])
    tot = sum(ss2[i] + ss2[4 + i] for i in range(4))
    tot = jnp.sum(jnp.where(diag(4 * rows, 0), tot, 0.0), axis=1, keepdims=True)
    r = lax.rsqrt(tot / (2 * d) + EPS)


    def renorm(c):
        for i in range(cw // 128):
            cols = pl.ds(pl.multiple_of(c * cw + i * 128, 128), 128)
            nv[:, cols] = (xnv[:, cols].astype(F32) * r * gv[1, pl.ds(c * (cw // 128) + i, 1), :]).astype(BF16)

    def qcopy(j):
        return pltpu.make_async_remote_copy(qown.at[j], qrec.at[j], c_sent.at[3], c_q.at[lax.div(j, 2)], partner, MESH)

    def fin(j):
        qout[:, pl.ds(pl.multiple_of(j * qw, 128), qw)] = (qown[j] + qrec[j]).astype(BF16)

    def q_pass(p, _):
        took(xnv.at[pl.ds(0, 3 * rows), pl.ds(0, d // 2)], c_x.at[p])
        loop(p * (ny // 2), (p + 1) * (ny // 2), renorm)
        ks = pl.ds(pl.multiple_of(p * (d // 2), 128), d // 2)

        def add(*js):
            @pl.when(p == 0)
            def _():
                for j in js:
                    wait(qk(j))

            for j in js:
                qown[j] = qown[j] + _dot(nv[:, ks], ring[lax.rem(j + ng + nm + 1, slots), ks])

            @pl.when(p == 1)
            def _():
                for j in js:
                    qcopy(j).start()

        def q_pair(i, _):
            add(2 * i, 2 * i + 1)
            return 0

        lax.fori_loop(0, nq // 2, q_pair, 0)
        add(nq - 1)
        return 0

    lax.fori_loop(0, 2, q_pass, 0)

    def fin_pair(i):
        took(qrec.at[pl.ds(0, 2)], c_q.at[i])
        fin(2 * i)
        fin(2 * i + 1)

    loop(0, nq // 2, fin_pair)
    took(qrec.at[0], c_q.at[nq // 2])
    fin(nq - 1)

    took(xnv.at[pl.ds(0, 3 * rows)], c_sent.at[2])
    took(qown, c_sent.at[3])


def _store(x_ref, q_ref, xo_hbm, qo_hbm, sem):
    cx = pltpu.make_async_copy(x_ref, xo_hbm, sem.at[0])
    cq = pltpu.make_async_copy(q_ref, qo_hbm, sem.at[1])
    cx.start()
    cq.start()
    cx.wait()
    cq.wait()


def solution(mesh):
    def body(x, g1, g2, w_gate, w_up, w_down, o, w_o, w_qkv):
        t, d = x.shape
        kd, ko, q = w_down.shape[0], w_o.shape[0], w_qkv.shape[1]
        slots, half, nm, cw, qw = 6, 384, 4, 256, 768
        ng, ny, nq, rows = (kd - nm * 256) // half, d // cw, q // qw, t // 4
        cfg = (d, kd, ko, slots, half, ng, nm, cw, ny, qw, nq, rows)
        dma = pltpu.SemaphoreType.DMA
        any_ = pl.BlockSpec(memory_space=pl.ANY)
        vmem = pl.BlockSpec(memory_space=pltpu.VMEM)
        outs = (jax.ShapeDtypeStruct((t, d), BF16), jax.ShapeDtypeStruct((t, q), BF16))
        mids = (pltpu.VMEM((t, d), BF16), pltpu.VMEM((t, q), BF16))
        res = pl.pallas_call(
            functools.partial(_kernel, cfg),
            out_shape=mids,
            in_specs=[any_] * 9,
            out_specs=(vmem, vmem),
            scratch_shapes=[
                pltpu.VMEM((slots, d, 2 * half), BF16),
                pltpu.VMEM((ny, ko + kd, cw), BF16),
                pltpu.VMEM((t, d), BF16),
                pltpu.VMEM((2, d // 128, 128), F32),
                pltpu.VMEM((t, ko + kd), BF16),
                pltpu.VMEM((t, d), BF16),
                pltpu.VMEM((2, t, 128), F32),
                pltpu.VMEM((8, 1, 128), F32),
                pltpu.VMEM((ng + nm + 1, t, 2 * half), F32),
                pltpu.VMEM((ng + nm + 1, t, 2 * half), F32),
                pltpu.VMEM((ny, t, cw), F32),
                pltpu.VMEM((3, ny, rows, cw), F32),
                pltpu.VMEM((nq, t, qw), F32),
                pltpu.VMEM((nq, t, qw), F32),
                dma((3,)), dma((slots,)), dma((ny,)),
                dma((2,)), dma((ng + nm + 1,)), dma((ny,)), dma((2,)), dma((1,)), dma(((nq + 1) // 2,)), dma((7,)),
            ],
            compiler_params=pltpu.CompilerParams(collective_id=0, has_side_effects=True,
                                                 vmem_limit_bytes=60_000_000),
            name='block',
        )(x, g1.reshape(-1, 128), g2.reshape(-1, 128), w_gate, w_up, w_down, o, w_o, w_qkv)
        return pl.pallas_call(_store, out_shape=outs, in_specs=[vmem, vmem], out_specs=(any_, any_),
                              scratch_shapes=[dma((2,))], name='store')(*[pltpu.with_memory_space_constraint(r, pltpu.VMEM) for r in res])

    in_specs = (P(None, 'h'), P('h'), P('h'), P('h', 'f'), P('h', 'f'), P('f', 'h'),
                P(None, 'f'), P('f', 'h'), P('h', 'f'))
    return jax.shard_map(body, mesh=mesh, in_specs=in_specs,
                         out_specs=(P(None, 'h'), P(None, 'f')), check_vma=False)
```

```python
import functools

import jax
import jax.numpy as jnp
from jax import lax
from jax.experimental import pallas as pl
from jax.experimental.pallas import tpu as pltpu
from jax.sharding import PartitionSpec as P

EPS = 1e-6
MESH = pl.DeviceIdType.MESH
F32, BF16 = jnp.float32, jnp.bfloat16


def _dot(a, b):
    return jnp.dot(a, b, preferred_element_type=F32)


def _kernel(cfg, x_hbm, g1_hbm, g2_hbm, wg_hbm, wu_hbm, wd_hbm, o_hbm, wo_hbm, wq_hbm,
            xnv, qout,
            ring, wdv, xv, gv, oa, nv, ss1, ss2, pown, prec, ysend, yrec, qown, qrec,
            s_in, s_w, s_dn,
            c_ss, c_p, c_y, c_x, c_s2, c_q, c_sent):
    d, kd, ko, slots, half, ng, nm, cw, ny, qw, nq, rows = cfg
    f, h = lax.axis_index('f'), lax.axis_index('h')
    partner = (f, 1 - h)
    fx = [f, f + 1 - 2 * lax.rem(f, 2), lax.rem(f + 2, 4), 3 - f]

    def small():
        return [pltpu.make_async_copy(x_hbm, xv, s_in.at[0]),
                pltpu.make_async_copy(g1_hbm, gv.at[0], s_in.at[1]),
                pltpu.make_async_copy(g2_hbm, gv.at[1], s_in.at[1]),
                pltpu.make_async_copy(o_hbm, oa.at[:, pl.ds(0, ko)], s_in.at[2])]

    def wide(j):
        return j, pl.multiple_of(j * half, 128), half

    def mid(m):
        return ng + m, pl.multiple_of(ng * half + m * 256, 128), 256

    last = (ng + nm, ng * half + nm * 256, 128)

    def gu(i, at, w):
        slot, cols = lax.rem(i, slots), pl.ds(at, w)
        return [pltpu.make_async_copy(wg_hbm.at[:, cols], ring.at[slot, :, pl.ds(0, w)], s_w.at[slot]),
                pltpu.make_async_copy(wu_hbm.at[:, cols], ring.at[slot, :, pl.ds(w, w)], s_w.at[slot])]

    def dn(c):
        cols = pl.ds(pl.multiple_of(c * cw, 128), cw)
        return [pltpu.make_async_copy(wo_hbm.at[:, cols], wdv.at[c, pl.ds(0, ko)], s_dn.at[lax.rem(c, ny // 2)]),
                pltpu.make_async_copy(wd_hbm.at[:, cols], wdv.at[c, pl.ds(ko, kd)], s_dn.at[lax.rem(c, ny // 2)])]

    def qk(j):
        slot, cols = lax.rem(j + ng + nm + 1, slots), pl.ds(pl.multiple_of(j * qw, 128), qw)
        return [pltpu.make_async_copy(wq_hbm.at[:, cols], ring.at[slot], s_w.at[slot])]

    def took(ref, sem):
        pltpu.make_async_copy(ref, ref, sem).wait()

    def start(copies, priority):
        for c in copies:
            c.start(priority=priority)

    def wait(copies):
        for c in copies:
            c.wait()

    def loop(lo, hi, fn):
        lax.fori_loop(lo, hi, lambda i, _: (fn(i), 0)[1], 0)

    ins = small()
    start(ins, 0)
    loop(0, ng, lambda j: start(gu(*wide(j)), 0))
    loop(0, ny // 2, lambda c: start(dn(c), 1))

    barrier = pltpu.get_barrier_semaphore()
    for k in range(4):
        for t in range(2):
            if k or t:
                pl.semaphore_signal(barrier, inc=1, device_id=(fx[k], h if t == 0 else 1 - h), device_id_type=MESH)

    took(xv, s_in.at[0])
    xf = xv[...].astype(F32)
    s = jnp.sum(xf * xf, axis=-1, keepdims=True)
    ss1[h] = jnp.broadcast_to(s, ss1.shape[1:])
    pl.semaphore_wait(barrier, 7)
    ex = pltpu.make_async_remote_copy(ss1.at[h], ss1.at[h], c_ss.at[0], c_ss.at[1], partner, MESH)
    ex.start()
    ex.wait()
    r = lax.rsqrt((ss1[0] + ss1[1])[:, :1] / (2 * d) + EPS)
    took(gv, s_in.at[1])
    for i in range(d // 128):
        cols = slice(i * 128, (i + 1) * 128)
        nv[:, cols] = (xv[:, cols].astype(F32) * r * gv[0, i:i + 1, :]).astype(BF16)

    def pcopy(i, w):
        part = pl.ds(0, 2 * w)
        return pltpu.make_async_remote_copy(pown.at[i, :, part], prec.at[i, :, part], c_sent.at[0], c_p.at[i], partner, MESH)

    def act(i, at, w):
        took(prec.at[i, :, pl.ds(0, 2 * w)], c_p.at[i])
        g = pown[i, :, :w] + prec[i, :, :w]
        u = pown[i, :, w:2 * w] + prec[i, :, w:2 * w]
        oa[:, pl.ds(pl.multiple_of(ko + at, 128), w)] = (g / (1.0 + jnp.exp(-g)) * u).astype(BF16)

    def product(i, at, w):
        slot, part = lax.rem(i, slots), pl.ds(0, 2 * w)
        took(ring.at[slot, :, part], s_w.at[slot])
        pown[i, :, part] = _dot(nv[...], ring[slot, :, part])
        pcopy(i, w).start()

    def gu_step(j, _):
        product(*wide(j))

        @pl.when(j < nm)
        def _():
            start(gu(*mid(j)), 0)

        @pl.when(j == nm)
        def _():
            start(gu(*last), 0)

        @pl.when(j > 1)
        def _():
            act(*wide(j - 2))
        return 0

    def mid_step(m, _):
        product(*mid(m))

        @pl.when(m < 2)
        def _():
            act(*wide(ng - 2 + m))
        return 0

    lax.fori_loop(0, ng, gu_step, 0)
    lax.fori_loop(0, nm, mid_step, 0)
    product(*last)

    blk = [pl.ds(pl.multiple_of(fx[k] * rows, rows), rows) for k in range(4)]
    mine = blk[0]

    def chunk(c):
        return pl.ds(pl.multiple_of(c * cw, 128), cw)

    def ycopy(c, k):
        return pltpu.make_async_remote_copy(ysend.at[c, blk[k]], yrec.at[k - 1, c], c_sent.at[1], c_y.at[lax.div(c, ny // 2) * (c - ny // 2 + 1)],
                                            (fx[k], h), MESH)

    def xcopy(c, k):
        at = xnv.at[mine, chunk(c)]
        return pltpu.make_async_remote_copy(at, at, c_sent.at[2], c_x.at[lax.div(c, ny // 2)], (fx[k], h), MESH)

    def spread(c):
        for k in (3, 1, 2):
            xcopy(c, k).start()

    def scatter(c):
        for k in (3, 1, 2):
            ycopy(c, k).start()

    loop(0, nm - 2, lambda m: act(*mid(m)))
    ins[3].wait()
    took(wdv.at[0], s_dn.at[0])
    start(dn(ny // 2), 1)
    kk = ko + ng * half + (nm - 2) * 256
    ysend[0] = _dot(oa[:, :kk], wdv[0, :kk])
    loop(nm - 2, nm, lambda m: act(*mid(m)))
    act(*last)
    ysend[0] = ysend[0] + _dot(oa[:, kk:], wdv[0, kk:])
    scatter(0)

    def dn_step(c, _):
        took(wdv.at[c], s_dn.at[lax.rem(c, ny // 2)])

        @pl.when(c < ny // 2)
        def _():
            start(dn(c + ny // 2), 1)

        @pl.when(c == ny // 2 - 1)
        def _():
            loop(0, nq, lambda j: start(qk(j), 1))

        ysend[c] = _dot(oa[...], wdv[c])
        scatter(c)
        return 0

    lax.fori_loop(1, ny, dn_step, 0)

    def block(c, s):
        @pl.when(c >= ny // 2)
        def _():
            took(yrec.at[:, c], c_y.at[c - ny // 2 + 1])

        y = (ysend[c, mine] + yrec[0, c]) + (yrec[1, c] + yrec[2, c])
        xn = (xv[mine, chunk(c)].astype(F32) + y).astype(BF16)
        xnv[mine, chunk(c)] = xn

        @pl.when(c < ny // 2)
        def _():
            spread(c)

        xf = xn.astype(F32)
        return s + jnp.sum(xf * xf, axis=-1, keepdims=True)

    took(yrec.at[:, pl.ds(0, ny // 2)], c_y.at[0])
    s = lax.fori_loop(0, ny, block, jnp.zeros((rows, 1), F32))

    def diag(n, first):
        i = lax.broadcasted_iota(jnp.int32, (n, 128), 0) + first
        return i == lax.broadcasted_iota(jnp.int32, (n, 128), 1)

    ss2[h * 4 + f] = jnp.sum(jnp.where(diag(rows, f * rows), s, 0.0), axis=0, keepdims=True)

    def scopy(k, t):
        return pltpu.make_async_remote_copy(ss2.at[h * 4 + f], ss2.at[h * 4 + f], c_sent.at[4], c_s2.at[0],
                                            (fx[k], h if t == 0 else 1 - h), MESH)

    peers = [(k, t) for k in (3, 1, 2, 0) for t in (0, 1) if k or t]
    for k, t in peers:
        scopy(k, t).start()
    loop(ny // 2, ny, spread)
    qown[...] = jnp.zeros_like(qown)
    took(pown.at[pl.ds(0, kd // half)], c_sent.at[0])
    took(ysend.at[:, pl.ds(0, 3 * rows)], c_sent.at[1])
    took(ss2.at[pl.ds(0, 7)], c_sent.at[4])
    took(ss2.at[pl.ds(0, 7)], c_s2.at[0])
    tot = sum(ss2[i] + ss2[4 + i] for i in range(4))
    tot = jnp.sum(jnp.where(diag(4 * rows, 0), tot, 0.0), axis=1, keepdims=True)
    r = lax.rsqrt(tot / (2 * d) + EPS)


    def renorm(c):
        for i in range(cw // 128):
            cols = pl.ds(pl.multiple_of(c * cw + i * 128, 128), 128)
            nv[:, cols] = (xnv[:, cols].astype(F32) * r * gv[1, pl.ds(c * (cw // 128) + i, 1), :]).astype(BF16)

    def qcopy(j):
        return pltpu.make_async_remote_copy(qown.at[j], qrec.at[j], c_sent.at[3], c_q.at[lax.div(j, 2)], partner, MESH)

    def fin(j):
        qout[:, pl.ds(pl.multiple_of(j * qw, 128), qw)] = (qown[j] + qrec[j]).astype(BF16)

    def q_pass(p, _):
        took(xnv.at[pl.ds(0, 3 * rows), pl.ds(0, d // 2)], c_x.at[p])
        loop(p * (ny // 2), (p + 1) * (ny // 2), renorm)
        ks = pl.ds(pl.multiple_of(p * (d // 2), 128), d // 2)

        def add(*js):
            @pl.when(p == 0)
            def _():
                for j in js:
                    wait(qk(j))

            for j in js:
                qown[j] = qown[j] + _dot(nv[:, ks], ring[lax.rem(j + ng + nm + 1, slots), ks])

            @pl.when(p == 1)
            def _():
                for j in js:
                    qcopy(j).start()

        def q_pair(i, _):
            add(2 * i, 2 * i + 1)
            return 0

        lax.fori_loop(0, nq // 2, q_pair, 0)
        add(nq - 1)
        return 0

    lax.fori_loop(0, 2, q_pass, 0)

    def fin_pair(i):
        took(qrec.at[pl.ds(0, 2)], c_q.at[i])
        fin(2 * i)
        fin(2 * i + 1)

    loop(0, nq // 2, fin_pair)
    took(qrec.at[0], c_q.at[nq // 2])
    fin(nq - 1)

    took(xnv.at[pl.ds(0, 3 * rows)], c_sent.at[2])
    took(qown, c_sent.at[3])


def _store(x_ref, q_ref, xo_hbm, qo_hbm, sem):
    cx = pltpu.make_async_copy(x_ref, xo_hbm, sem.at[0])
    cq = pltpu.make_async_copy(q_ref, qo_hbm, sem.at[1])
    cx.start()
    cq.start()
    cx.wait()
    cq.wait()


def solution(mesh):
    def body(x, g1, g2, w_gate, w_up, w_down, o, w_o, w_qkv):
        t, d = x.shape
        kd, ko, q = w_down.shape[0], w_o.shape[0], w_qkv.shape[1]
        slots, half, nm, cw, qw = 6, 384, 4, 256, 768
        ng, ny, nq, rows = (kd - nm * 256) // half, d // cw, q // qw, t // 4
        cfg = (d, kd, ko, slots, half, ng, nm, cw, ny, qw, nq, rows)
        dma = pltpu.SemaphoreType.DMA
        any_ = pl.BlockSpec(memory_space=pl.ANY)
        vmem = pl.BlockSpec(memory_space=pltpu.VMEM)
        outs = (jax.ShapeDtypeStruct((t, d), BF16), jax.ShapeDtypeStruct((t, q), BF16))
        mids = (pltpu.VMEM((t, d), BF16), pltpu.VMEM((t, q), BF16))
        res = pl.pallas_call(
            functools.partial(_kernel, cfg),
            out_shape=mids,
            in_specs=[any_] * 9,
            out_specs=(vmem, vmem),
            scratch_shapes=[
                pltpu.VMEM((slots, d, 2 * half), BF16),
                pltpu.VMEM((ny, ko + kd, cw), BF16),
                pltpu.VMEM((t, d), BF16),
                pltpu.VMEM((2, d // 128, 128), F32),
                pltpu.VMEM((t, ko + kd), BF16),
                pltpu.VMEM((t, d), BF16),
                pltpu.VMEM((2, t, 128), F32),
                pltpu.VMEM((8, 1, 128), F32),
                pltpu.VMEM((ng + nm + 1, t, 2 * half), F32),
                pltpu.VMEM((ng + nm + 1, t, 2 * half), F32),
                pltpu.VMEM((ny, t, cw), F32),
                pltpu.VMEM((3, ny, rows, cw), F32),
                pltpu.VMEM((nq, t, qw), F32),
                pltpu.VMEM((nq, t, qw), F32),
                dma((3,)), dma((slots,)), dma((ny // 2,)),
                dma((2,)), dma((ng + nm + 1,)), dma((ny - ny // 2 + 1,)), dma((2,)), dma((1,)), dma(((nq + 1) // 2,)), dma((5,)),
            ],
            compiler_params=pltpu.CompilerParams(collective_id=0, has_side_effects=True,
                                                 vmem_limit_bytes=60_000_000),
            name='block',
        )(x, g1.reshape(-1, 128), g2.reshape(-1, 128), w_gate, w_up, w_down, o, w_o, w_qkv)
        return pl.pallas_call(_store, out_shape=outs, in_specs=[vmem, vmem], out_specs=(any_, any_),
                              scratch_shapes=[dma((2,))], name='store')(*[pltpu.with_memory_space_constraint(r, pltpu.VMEM) for r in res])

    in_specs = (P(None, 'h'), P('h'), P('h'), P('h', 'f'), P('h', 'f'), P('f', 'h'),
                P(None, 'f'), P('f', 'h'), P('h', 'f'))
    return jax.shard_map(body, mesh=mesh, in_specs=in_specs,
                         out_specs=(P(None, 'h'), P(None, 'f')), check_vma=False)
```

```python
import functools

import jax
import jax.numpy as jnp
from jax import lax
from jax.experimental import pallas as pl
from jax.experimental.pallas import tpu as pltpu
from jax.sharding import PartitionSpec as P

EPS = 1e-6
MESH = pl.DeviceIdType.MESH
F32, BF16 = jnp.float32, jnp.bfloat16


def _dot(a, b):
    return jnp.dot(a, b, preferred_element_type=F32)


def _kernel(cfg, x_hbm, g1_hbm, g2_hbm, wg_hbm, wu_hbm, wd_hbm, o_hbm, wo_hbm, wq_hbm,
            xnv, qout,
            ring, wdv, xv, gv, oa, nv, ss1, ss2, pown, prec, ysend, yrec, qown, qrec,
            s_in, s_w, s_dn,
            c_ss, c_p, c_y, c_x, c_s2, c_q, c_sent):
    d, kd, ko, slots, half, ng, nm, cw, ny, qw, nq, rows = cfg
    f, h = lax.axis_index('f'), lax.axis_index('h')
    partner = (f, 1 - h)
    fx = [f, f + 1 - 2 * lax.rem(f, 2), lax.rem(f + 2, 4), 3 - f]

    def small():
        return [pltpu.make_async_copy(x_hbm, xv, s_in.at[0]),
                pltpu.make_async_copy(g1_hbm, gv.at[0], s_in.at[1]),
                pltpu.make_async_copy(g2_hbm, gv.at[1], s_in.at[1]),
                pltpu.make_async_copy(o_hbm, oa.at[:, pl.ds(0, ko)], s_in.at[2])]

    def wide(j):
        return j, pl.multiple_of(j * half, 128), half

    def mid(m):
        return ng + m, pl.multiple_of(ng * half + m * 256, 128), 256

    last = (ng + nm, ng * half + nm * 256, 128)

    def gu(i, at, w):
        slot, cols = lax.rem(i, slots), pl.ds(at, w)
        return [pltpu.make_async_copy(wg_hbm.at[:, cols], ring.at[slot, :, pl.ds(0, w)], s_w.at[slot]),
                pltpu.make_async_copy(wu_hbm.at[:, cols], ring.at[slot, :, pl.ds(w, w)], s_w.at[slot])]

    def dn(c):
        cols = pl.ds(pl.multiple_of(c * cw, 128), cw)
        return [pltpu.make_async_copy(wo_hbm.at[:, cols], wdv.at[c, pl.ds(0, ko)], s_dn.at[lax.rem(c, ny // 2)]),
                pltpu.make_async_copy(wd_hbm.at[:, cols], wdv.at[c, pl.ds(ko, kd)], s_dn.at[lax.rem(c, ny // 2)])]

    def qk(j):
        slot, cols = lax.rem(j + ng + nm + 1, slots), pl.ds(pl.multiple_of(j * qw, 128), qw)
        return [pltpu.make_async_copy(wq_hbm.at[:, cols], ring.at[slot], s_w.at[slot])]

    def took(ref, sem):
        pltpu.make_async_copy(ref, ref, sem).wait()

    def start(copies, priority):
        for c in copies:
            c.start(priority=priority)

    def wait(copies):
        for c in copies:
            c.wait()

    def loop(lo, hi, fn):
        lax.fori_loop(lo, hi, lambda i, _: (fn(i), 0)[1], 0)

    ins = small()
    start(ins, 0)
    loop(0, ng, lambda j: start(gu(*wide(j)), 0))
    loop(0, ny // 2, lambda c: start(dn(c), 1))

    barrier = pltpu.get_barrier_semaphore()
    for k in range(4):
        for t in range(2):
            if k or t:
                pl.semaphore_signal(barrier, inc=1, device_id=(fx[k], h if t == 0 else 1 - h), device_id_type=MESH)

    took(xv, s_in.at[0])
    xf = xv[...].astype(F32)
    s = jnp.sum(xf * xf, axis=-1, keepdims=True)
    ss1[h] = jnp.broadcast_to(s, ss1.shape[1:])
    pl.semaphore_wait(barrier, 7)
    ex = pltpu.make_async_remote_copy(ss1.at[h], ss1.at[h], c_ss.at[0], c_ss.at[1], partner, MESH)
    ex.start()
    ex.wait()
    r = lax.rsqrt((ss1[0] + ss1[1])[:, :1] / (2 * d) + EPS)
    took(gv, s_in.at[1])
    for i in range(d // 128):
        cols = slice(i * 128, (i + 1) * 128)
        nv[:, cols] = (xv[:, cols].astype(F32) * r * gv[0, i:i + 1, :]).astype(BF16)

    def pcopy(i, w):
        part = pl.ds(0, 2 * w)
        return pltpu.make_async_remote_copy(pown.at[i, :, part], prec.at[i, :, part], c_sent.at[0], c_p.at[i], partner, MESH)

    def act(i, at, w):
        took(prec.at[i, :, pl.ds(0, 2 * w)], c_p.at[i])
        g = pown[i, :, :w] + prec[i, :, :w]
        u = pown[i, :, w:2 * w] + prec[i, :, w:2 * w]
        oa[:, pl.ds(pl.multiple_of(ko + at, 128), w)] = (g / (1.0 + jnp.exp(-g)) * u).astype(BF16)

    def product(i, at, w):
        slot, part = lax.rem(i, slots), pl.ds(0, 2 * w)
        took(ring.at[slot, :, part], s_w.at[slot])
        pown[i, :, part] = _dot(nv[...], ring[slot, :, part])
        pcopy(i, w).start()

    def gu_step(j, _):
        product(*wide(j))

        @pl.when(j < nm)
        def _():
            start(gu(*mid(j)), 0)

        @pl.when(j == nm)
        def _():
            start(gu(*last), 0)

        @pl.when(j > 1)
        def _():
            act(*wide(j - 2))
        return 0

    def mid_step(m, _):
        product(*mid(m))

        @pl.when(m < 2)
        def _():
            act(*wide(ng - 2 + m))
        return 0

    lax.fori_loop(0, ng, gu_step, 0)
    lax.fori_loop(0, nm, mid_step, 0)
    product(*last)

    blk = [pl.ds(pl.multiple_of(fx[k] * rows, rows), rows) for k in range(4)]
    mine = blk[0]

    def chunk(c):
        return pl.ds(pl.multiple_of(c * cw, 128), cw)

    def ycopy(c, k):
        return pltpu.make_async_remote_copy(ysend.at[c, blk[k]], yrec.at[k - 1, c], c_sent.at[1], c_y.at[lax.div(c, ny // 2) * (c - ny // 2 + 1)],
                                            (fx[k], h), MESH)

    def xcopy(c, k):
        at = xnv.at[mine, chunk(c)]
        return pltpu.make_async_remote_copy(at, at, c_sent.at[2], c_x.at[lax.div(c, ny // 2)], (fx[k], h), MESH)

    def spread(c):
        for k in (3, 1, 2):
            xcopy(c, k).start()

    def scatter(c):
        for k in (3, 1, 2):
            ycopy(c, k).start()

    loop(0, nm - 2, lambda m: act(*mid(m)))
    ins[3].wait()
    took(wdv.at[0], s_dn.at[0])
    start(dn(ny // 2), 1)
    kk = ko + ng * half + (nm - 2) * 256
    ysend[0] = _dot(oa[:, :kk], wdv[0, :kk])
    loop(nm - 2, nm, lambda m: act(*mid(m)))
    act(*last)
    ysend[0] = ysend[0] + _dot(oa[:, kk:], wdv[0, kk:])
    scatter(0)

    def dn_step(c, _):
        took(wdv.at[c], s_dn.at[lax.rem(c, ny // 2)])

        @pl.when(c < ny // 2)
        def _():
            start(dn(c + ny // 2), 1)

        @pl.when(c == ny // 2 - 1)
        def _():
            loop(0, nq, lambda j: start(qk(j), 1))

        ysend[c] = _dot(oa[...], wdv[c])
        scatter(c)
        return 0

    lax.fori_loop(1, ny, dn_step, 0)

    def block(c, s):
        @pl.when(c >= ny // 2)
        def _():
            took(yrec.at[:, c], c_y.at[c - ny // 2 + 1])

        y = (ysend[c, mine] + yrec[0, c]) + (yrec[1, c] + yrec[2, c])
        xn = (xv[mine, chunk(c)].astype(F32) + y).astype(BF16)
        xnv[mine, chunk(c)] = xn

        @pl.when(c < ny // 2)
        def _():
            spread(c)

        xf = xn.astype(F32)
        return s + jnp.sum(xf * xf, axis=-1, keepdims=True)

    took(yrec.at[:, pl.ds(0, ny // 2)], c_y.at[0])
    s = lax.fori_loop(0, ny, block, jnp.zeros((rows, 1), F32))

    def diag(n, first):
        i = lax.broadcasted_iota(jnp.int32, (n, 128), 0) + first
        return i == lax.broadcasted_iota(jnp.int32, (n, 128), 1)

    ss2[h * 4 + f] = jnp.sum(jnp.where(diag(rows, f * rows), s, 0.0), axis=0, keepdims=True)

    def scopy(k, t):
        return pltpu.make_async_remote_copy(ss2.at[h * 4 + f], ss2.at[h * 4 + f], c_sent.at[4], c_s2.at[0],
                                            (fx[k], h if t == 0 else 1 - h), MESH)

    peers = [(k, t) for k in (3, 1, 2, 0) for t in (0, 1) if k or t]
    for k, t in peers:
        scopy(k, t).start()
    loop(ny // 2, ny, spread)
    qown[...] = jnp.zeros_like(qown)
    took(pown.at[pl.ds(0, kd // half)], c_sent.at[0])
    took(ysend.at[:, pl.ds(0, 3 * rows)], c_sent.at[1])
    took(ss2.at[pl.ds(0, 7)], c_sent.at[4])
    took(ss2.at[pl.ds(0, 7)], c_s2.at[0])
    tot = sum(ss2[i] + ss2[4 + i] for i in range(4))
    tot = jnp.sum(jnp.where(diag(4 * rows, 0), tot, 0.0), axis=1, keepdims=True)
    r = lax.rsqrt(tot / (2 * d) + EPS)


    def renorm(c):
        for i in range(cw // 128):
            cols = pl.ds(pl.multiple_of(c * cw + i * 128, 128), 128)
            nv[:, cols] = (xnv[:, cols].astype(F32) * r * gv[1, pl.ds(c * (cw // 128) + i, 1), :]).astype(BF16)

    def qcopy(j):
        return pltpu.make_async_remote_copy(qown.at[j], qrec.at[j], c_sent.at[3], c_q.at[lax.div(j, 2)], partner, MESH)

    def fin(j):
        qout[:, pl.ds(pl.multiple_of(j * qw, 128), qw)] = (qown[j] + qrec[j]).astype(BF16)

    def q_pass(p, _):
        took(xnv.at[pl.ds(0, 3 * rows), pl.ds(0, d // 2)], c_x.at[p])
        loop(p * (ny // 2), (p + 1) * (ny // 2), renorm)
        ks = pl.ds(pl.multiple_of(p * (d // 2), 128), d // 2)

        def add(*js):
            @pl.when(p == 0)
            def _():
                for j in js:
                    wait(qk(j))

            for j in js:
                qown[j] = qown[j] + _dot(nv[:, ks], ring[lax.rem(j + ng + nm + 1, slots), ks])

            @pl.when(p == 1)
            def _():
                for j in js:
                    qcopy(j).start()

        def q_pair(i, _):
            add(2 * i, 2 * i + 1)
            return 0

        lax.fori_loop(0, nq // 2, q_pair, 0)
        add(nq - 1)
        return 0

    lax.fori_loop(0, 2, q_pass, 0)

    def fin_pair(i):
        took(qrec.at[pl.ds(0, 2)], c_q.at[i])
        fin(2 * i)
        fin(2 * i + 1)

    loop(0, nq // 2, fin_pair)
    took(qrec.at[0], c_q.at[nq // 2])
    fin(nq - 1)

    took(xnv.at[pl.ds(0, 3 * rows)], c_sent.at[2])
    took(qown, c_sent.at[3])


def _store(x_ref, q_ref, xo_hbm, qo_hbm, sem):
    cx = pltpu.make_async_copy(x_ref, xo_hbm, sem.at[0])
    cq = pltpu.make_async_copy(q_ref, qo_hbm, sem.at[1])
    cq.start()
    cx.start()
    cx.wait()
    cq.wait()


def solution(mesh):
    def body(x, g1, g2, w_gate, w_up, w_down, o, w_o, w_qkv):
        t, d = x.shape
        kd, ko, q = w_down.shape[0], w_o.shape[0], w_qkv.shape[1]
        slots, half, nm, cw, qw = 6, 384, 4, 256, 768
        ng, ny, nq, rows = (kd - nm * 256) // half, d // cw, q // qw, t // 4
        cfg = (d, kd, ko, slots, half, ng, nm, cw, ny, qw, nq, rows)
        dma = pltpu.SemaphoreType.DMA
        any_ = pl.BlockSpec(memory_space=pl.ANY)
        vmem = pl.BlockSpec(memory_space=pltpu.VMEM)
        outs = (jax.ShapeDtypeStruct((t, d), BF16), jax.ShapeDtypeStruct((t, q), BF16))
        mids = (pltpu.VMEM((t, d), BF16), pltpu.VMEM((t, q), BF16))
        res = pl.pallas_call(
            functools.partial(_kernel, cfg),
            out_shape=mids,
            in_specs=[any_] * 9,
            out_specs=(vmem, vmem),
            scratch_shapes=[
                pltpu.VMEM((slots, d, 2 * half), BF16),
                pltpu.VMEM((ny, ko + kd, cw), BF16),
                pltpu.VMEM((t, d), BF16),
                pltpu.VMEM((2, d // 128, 128), F32),
                pltpu.VMEM((t, ko + kd), BF16),
                pltpu.VMEM((t, d), BF16),
                pltpu.VMEM((2, t, 128), F32),
                pltpu.VMEM((8, 1, 128), F32),
                pltpu.VMEM((ng + nm + 1, t, 2 * half), F32),
                pltpu.VMEM((ng + nm + 1, t, 2 * half), F32),
                pltpu.VMEM((ny, t, cw), F32),
                pltpu.VMEM((3, ny, rows, cw), F32),
                pltpu.VMEM((nq, t, qw), F32),
                pltpu.VMEM((nq, t, qw), F32),
                dma((3,)), dma((slots,)), dma((ny // 2,)),
                dma((2,)), dma((ng + nm + 1,)), dma((ny - ny // 2 + 1,)), dma((2,)), dma((1,)), dma(((nq + 1) // 2,)), dma((5,)),
            ],
            compiler_params=pltpu.CompilerParams(collective_id=0, has_side_effects=True,
                                                 vmem_limit_bytes=60_000_000),
            name='block',
        )(x, g1.reshape(-1, 128), g2.reshape(-1, 128), w_gate, w_up, w_down, o, w_o, w_qkv)
        return pl.pallas_call(_store, out_shape=outs, in_specs=[vmem, vmem], out_specs=(any_, any_),
                              scratch_shapes=[dma((2,))], name='store')(*[pltpu.with_memory_space_constraint(r, pltpu.VMEM) for r in res])

    in_specs = (P(None, 'h'), P('h'), P('h'), P('h', 'f'), P('h', 'f'), P('f', 'h'),
                P(None, 'f'), P('f', 'h'), P('h', 'f'))
    return jax.shard_map(body, mesh=mesh, in_specs=in_specs,
                         out_specs=(P(None, 'h'), P(None, 'f')), check_vma=False)
```
